512 devices in a mesh: rep: 8 (over y), dp: 64 (over z, x, core).
Axes of the slice: x: 4, y: 8, z: 8, core: 2. Of those that a mesh axis runs over, the one named last changes fastest.
Arguments:
- hidden: bfloat16 [1024, 2, 3584], P(('rep', 'dp')), may hold values from -96 to 96
- lm_head: bfloat16 [3584, 196608], P(None, ('rep', 'dp')), may hold values from -0.3125 to 0.3125
- reward_head: bfloat16 [3584], replicated, may hold values from -0.09375 to 0.09375
- target_ids: int32 [1024, 2], P(('rep', 'dp')), may hold values from 0 to 196607
- lengths: int32 [1024], P(('rep', 'dp')), may hold values from 1 to 2
- prompt_ids: int32 [1024], P(('rep', 'dp')), may hold values from 0 to 63, as said below
Outputs:
- token_logprobs: float32 [1024, 2], P(('rep', 'dp'))
- advantages: float32 [1024], P(('rep', 'dp'))
The draws below stay inside these ranges and needn't reach their ends.
Inputs may be any that keep to these rules, and one draw needn't show every extreme that they name: `prompt_ids`: each prompt id names exactly 16 responses.
All inputs are finite; a program needn't handle non-finite values.
Results may differ from the reference program's by a relative error of at most 0.0003.
Values may be sent and summed in bfloat16 or wider, within the bound.
A program may use at most 128 MiB of HBM per device.

```python
import jax
import jax.numpy as jnp
from jax import lax

D = 3584
VOC_DEV = 384
GROUP = 16
WIN = 2
VOCAB = 196608
PROMPTS = 64
RESPONSES = 1024
TOKENS = 2048


def draw_hidden(key, part):
    base = jax.random.truncated_normal(key, -6.0, 6.0, (RESPONSES, WIN, D), jnp.float32)
    return base.astype(jnp.bfloat16)


def draw_prompt_ids(key, part):
    order = jax.random.permutation(jax.random.fold_in(key, 5), RESPONSES)
    return (order // GROUP).astype(jnp.int32)


def plant(entries, key, smallest, top_value):
    longest = entries.shape.index(max(entries.shape))
    spots = []
    for shift in (0, 1):
        where = [jax.random.randint(jax.random.fold_in(key, axis), (), 0, length) for axis, length in enumerate(entries.shape)]
        where[longest] = (where[longest] + shift) % entries.shape[longest]
        spots.append(tuple(where))
    return entries.at[spots[0]].set(smallest).at[spots[1]].set(top_value)


def levels(own_key, extent, split, low, top_value):
    level = 1.0
    for position, blocks in split:
        heights = jax.random.uniform(jax.random.fold_in(jax.random.fold_in(own_key, 6), position), (blocks,), jnp.float32, low / len(split), top_value / len(split))
        level = level * jnp.repeat(jnp.exp(heights), extent[position] // blocks).reshape((-1,) + (1,) * (len(extent) - 1 - position))
    return level


def centred(rng, extent, scale, limit, pieces=(), kind=jnp.bfloat16):
    array = jax.random.normal(rng, extent, jnp.float32) * scale
    if len(pieces) > 0:
        array = levels(rng, extent, pieces, -0.22, 0.18) * array
    return jnp.clip(array, min=-limit, max=limit).astype(kind)


def setup_inputs(seed: int = 0) -> dict:
    keys = jax.random.split(jax.random.key(seed), 7)
    hidden = draw_hidden(jax.random.fold_in(keys[6], 71), 0)
    lm_head = centred(keys[1], (D, VOCAB), (D // 9) ** -0.5, 0.3125, ((1, 512),))
    reward_head = centred(keys[2], (D,), D ** -0.5, 0.09375)
    target_ids = plant(jax.random.randint(keys[3], (RESPONSES, WIN), 0, VOCAB), jax.random.fold_in(keys[3], 1), 0, VOCAB - 1).astype(jnp.int32)
    lengths = plant(jax.random.randint(keys[4], (RESPONSES,), 1, WIN + 1), jax.random.fold_in(keys[4], 1), 1, WIN).astype(jnp.int32)
    prompt_ids = draw_prompt_ids(jax.random.fold_in(keys[6], 71), 0)
    return dict(hidden=hidden, lm_head=lm_head, reward_head=reward_head, target_ids=target_ids, lengths=lengths, prompt_ids=prompt_ids)


def reference(hidden, lm_head, reward_head, target_ids, lengths, prompt_ids):
    rows = hidden.reshape(TOKENS, D)
    wanted = target_ids.reshape(TOKENS)
    block = VOC_DEV * 8
    count = VOCAB // block

    def sweep(carry, index):
        peak, total, picked = carry
        start = (index * block).astype(jnp.int32)
        weights = lax.dynamic_slice_in_dim(lm_head, start, block, 1)
        logits = jnp.dot(rows, weights, preferred_element_type=jnp.float32)
        fresh = jnp.maximum(peak, lax.optimization_barrier(jnp.max(logits, axis=1)))
        total = total * jnp.exp(peak - fresh) + lax.optimization_barrier(jnp.sum(jnp.exp(logits - fresh[:, None]), axis=1))
        columns = start + lax.broadcasted_iota(jnp.int32, (1, block), 1)
        picked = picked + lax.optimization_barrier(jnp.sum(jnp.where(columns == wanted[:, None], logits, 0.0), axis=1))
        return ((fresh, total, picked), None)
    zeros = jnp.zeros((TOKENS,), jnp.float32)
    start_carry = (jnp.full((TOKENS,), -jnp.inf, jnp.float32), zeros, zeros)
    (peak, total, picked), _ = lax.scan(sweep, start_carry, jnp.arange(count, dtype=jnp.int32))
    logprob = (picked - (peak + jnp.log(total))).reshape(RESPONSES, WIN)
    positions = lax.broadcasted_iota(jnp.int32, (RESPONSES, WIN), 1)
    token_logprobs = jnp.where(positions < lengths[:, None], logprob, 0.0)
    last = jnp.take_along_axis(hidden, (lengths - 1).astype(jnp.int32)[:, None, None], axis=1)[:, 0, :]
    rewards = jnp.dot(last, reward_head, preferred_element_type=jnp.float32)
    member = (prompt_ids[:, None] == lax.broadcasted_iota(jnp.int32, (1, PROMPTS), 1)).astype(jnp.float32)
    sums = jnp.dot(rewards, member, precision=lax.Precision.HIGHEST)
    squares = jnp.dot(rewards * rewards, member, precision=lax.Precision.HIGHEST)
    means = sums / GROUP
    scales = jnp.sqrt(jnp.maximum(squares / GROUP - means * means, 1.0))
    centre = jnp.dot(member, means, precision=lax.Precision.HIGHEST)
    spread = jnp.dot(member, scales, precision=lax.Precision.HIGHEST)
    advantages = (rewards - centre) / spread
    return (token_logprobs, advantages)
```

```python
import functools

import jax
import jax.numpy as jnp
from jax import lax
from jax.experimental import pallas as pl
from jax.experimental.pallas import tpu as pltpu
from jax.sharding import Mesh
from jax.sharding import PartitionSpec as P

GROUP = 16
PROMPTS = 64
REP_DP = ("rep", "dp_0", "dp_1", "dp_2")
AXY, AXZ, AXX, AXC = REP_DP
LANES = 128
MESH = pl.DeviceIdType.MESH
F32 = jnp.float32


def ring_offsets(n):
    order = [0]
    for d in range(1, n // 2 + 1):
        order.append(-d)
        if 2 * d < n:
            order.append(d)
    return order


def hops(n, off):
    return min(off % n, -off % n)


def first_events(n):
    out = []
    for d in range(1, n // 2 + 1):
        out.append((d, 1))
        if 2 * d < n:
            out.append((d, -1))
    return out


def second_events(n1, n2):
    out = []
    for j in range(n1):
        for d in range(1, n2 // 2 + 1):
            if 2 * d < n2:
                out.append((j, d, 1))
                out.append((j, d, -1))
            else:
                out.append((j, d, 1 if j % 2 == 0 else -1))
    return out


def kernel(
    sizes, hid, whbm, rhead, ids, lens, pids, out1, out2,
    wmat, abuf, bbuf, acc, gath, gmeta, meta, tiles, got_z, got_y, got_x, sum_y, sum_x, pair, pgot,
    own_sem, w_send, w_recv, g_send, g_recv, m_send, m_recv, p_send, p_recv,
    a_send, a_recv, b_send, b_recv, z_send, z_recv, y_send, y_recv, x_send, x_recv,
):
    nx, ny, nz, ka, kb = sizes
    rows = nx * 4
    voc = whbm.shape[1]
    y, z, x, c = (lax.axis_index(a) for a in (AXY, AXZ, AXX, AXC))

    def at(pos, off, n):
        return lax.rem(pos + (off % n), n)

    own_w = pltpu.make_async_copy(whbm, wmat.at[:, pl.ds(0, voc)], own_sem)
    own_w.start()

    row8 = lax.broadcasted_iota(jnp.int32, (8, LANES), 0)
    lane8 = lax.broadcasted_iota(jnp.int32, (8, LANES), 1)
    idv = jnp.zeros((8, LANES), jnp.int32)
    for t in range(4):
        idv = jnp.where(row8 == t, ids[t // 2, t % 2], idv)
    digits = jnp.where(lane8 == 0, idv >> 16, jnp.where(lane8 == 1, (idv >> 8) & 255, idv & 255))
    meta[...] = jnp.where(lane8 < 3, digits, 0).astype(F32)

    barrier = pltpu.get_barrier_semaphore()
    partners = [{AXX: at(x, d, nx)} for d in range(1, nx)]
    partners += [{AXY: at(y, d, ny)} for d in (1, -1)]
    partners += [{AXZ: at(z, d, nz)} for d in (1, -1)]
    partners += [{AXC: 1 - c}]
    for dev in partners:
        pl.semaphore_signal(barrier, inc=1, device_id=dev, device_id_type=MESH)
    pl.semaphore_wait(barrier, len(partners))

    started = []

    def send(src, dst, ssem, rsem, dev):
        copy = pltpu.make_async_remote_copy(
            src_ref=src, dst_ref=dst, send_sem=ssem, recv_sem=rsem, device_id=dev, device_id_type=MESH
        )
        copy.start()
        started.append(copy)
        return copy

    for d in range(1, nx):
        send(hid, gath.at[x], g_send.at[d - 1], g_recv.at[d - 1], {AXX: at(x, d, nx)})
    for d in range(1, nx):
        send(meta, gmeta.at[x], m_send.at[d - 1], m_recv.at[d - 1], {AXX: at(x, d, nx)})
    send(whbm, wmat.at[:, pl.ds(voc, voc)], w_send, w_recv, {AXC: 1 - c})

    gath[x] = hid[...]
    gmeta[x] = meta[...]

    weight = rhead[...].astype(F32)
    rewards = []
    for r in range(2):
        both = jnp.sum(hid[r].astype(F32) * weight, axis=1, keepdims=True)
        rewards.append(jnp.where(lens[r] == 1, both[0:1], both[1:2]))
    lane1 = lax.broadcasted_iota(jnp.int32, (1, LANES), 1)
    stacked = jnp.zeros((1, LANES), F32)
    for r in range(2):
        stacked += jnp.where(lane1 == pids[r], rewards[r], 0.0)
        stacked += jnp.where(lane1 == pids[r] + PROMPTS, rewards[r] * rewards[r], 0.0)
    pair[...] = jnp.where(row8 == 3, stacked, 0.0)

    for d in range(1, nx):
        src = at(x, -d, nx)
        pltpu.make_async_copy(gath.at[src], gath.at[src], g_recv.at[d - 1]).wait()
        pltpu.make_async_copy(gmeta.at[src], gmeta.at[src], m_recv.at[d - 1]).wait()

    whole = jnp.concatenate(
        [gath[i, r].astype(F32) for i in range(nx) for r in range(2)], axis=0
    ).astype(jnp.bfloat16)
    for k in range(ka):
        abuf[y, z, k] = whole[:, k * LANES:(k + 1) * LANES]
    for k in range(kb):
        bbuf[y, z, k] = whole[:, (ka + k) * LANES:(ka + k + 1) * LANES]
    abuf[y, z, ka] = jnp.concatenate([gmeta[i, 0:4] for i in range(nx)], axis=0).astype(jnp.bfloat16)

    send(pair, pgot, p_send, p_recv, {AXC: 1 - c})

    class Colour:
        pass

    def colour(buf, first, p1, n1, axis1, p2, n2, axis2, ssem, rsem):
        col = Colour()
        offs = ring_offsets(n1)
        ev1, ev2 = first_events(n1), second_events(n1, n2)
        index1 = {e: i for i, e in enumerate(ev1)}
        index2 = {e: len(ev1) + i for i, e in enumerate(ev2)}

        def block(off1, off2):
            q1, q2 = at(p1, off1, n1), at(p2, off2, n2)
            return buf.at[q1, q2] if first else buf.at[q2, q1]

        def put1(d, way):
            if (d, way) in index1:
                i = index1[(d, way)]
                b = block(-way * (d - 1), 0)
                send(b, b, ssem.at[i], rsem.at[i], {axis1: at(p1, way, n1)})

        def put2(j, d, way):
            if (j, d, way) in index2:
                i = index2[(j, d, way)]
                b = block(offs[j], -way * (d - 1))
                send(b, b, ssem.at[i], rsem.at[i], {axis2: at(p2, way, n2)})

        def take(b, i):
            pltpu.make_async_copy(b, b, rsem.at[i]).wait()

        def begin():
            for way in (1, -1):
                put1(1, way)
            for way in (1, -1):
                put2(0, 1, way)

        def got1(d, way):
            take(block(-way * d, 0), index1[(d, way)])
            put1(d + 1, way)
            j = [o % n1 for o in offs].index(-way * d % n1)
            for w2 in (1, -1):
                put2(j, 1, w2)

        def got2(j, d, way):
            take(block(offs[j], -way * d), index2[(j, d, way)])
            put2(j, d + 1, way)

        col.begin = begin
        col.events = [(e[0], 0, functools.partial(got1, *e)) for e in ev1]
        col.events += [
            (hops(n1, offs[e[0]]) + e[1], 1, functools.partial(got2, *e))
            for e in sorted(ev2, key=lambda e: (hops(n1, offs[e[0]]) + e[1], e[1], e[0]))
        ]
        return col

    first = colour(abuf, True, y, ny, AXY, z, nz, AXZ, a_send, a_recv)
    second = colour(bbuf, False, z, nz, AXZ, y, ny, AXY, b_send, b_recv)
    first.begin()
    second.begin()
    acc[...] = jnp.zeros_like(acc)

    wide = 2 * LANES if (2 * voc) % (2 * LANES) == 0 else LANES

    def multiply(is_first, positions):
        buf, nk, k0, n1 = (abuf, ka, 0, ny) if is_first else (bbuf, kb, ka, nz)

        def step(n, carry):
            cols = pl.ds(pl.multiple_of(n * wide, wide), wide)
            left = []
            for q in positions:
                parts = [
                    (buf[:, q, k] if is_first else buf[q, :, k]).reshape(n1 * rows, LANES)
                    for k in range(nk)
                ]
                left.append(jnp.concatenate(parts, axis=1))
            left = jnp.concatenate(left, axis=0) if len(left) > 1 else left[0]
            right = wmat[pl.ds(k0 * LANES, nk * LANES), cols]
            part = jnp.dot(left, right, preferred_element_type=F32)
            for i, q in enumerate(positions):
                piece = part[i * n1 * rows:(i + 1) * n1 * rows].reshape(n1, rows, wide)
                if is_first:
                    acc[:, q, :, cols] += piece
                else:
                    acc[q, :, :, cols] += piece
            return carry

        lax.fori_loop(0, 2 * voc // wide, step, 0)

    waves = ny // 2 + nz // 2
    waited = False
    for wave in range(1, waves + 1):
        for kind in (0, 1):
            mine = [[e for e in col.events if e[0] == wave and e[1] == kind] for col in (first, second)]
            for i in range(max(len(m) for m in mine)):
                for m in mine:
                    if i < len(m):
                        m[i][2]()
        for is_first, n1, n2, p2 in ((True, ny, nz, z), (False, nz, ny, y)):
            d = wave - n1 // 2
            if 0 <= d <= n2 // 2:
                if not waited:
                    own_w.wait()
                    pltpu.make_async_copy(whbm, wmat.at[:, pl.ds(voc, voc)], w_recv).wait()
                    waited = True
                where = [at(p2, d, n2)]
                if 0 < d and 2 * d < n2:
                    where.append(at(p2, -d, n2))
                multiply(is_first, where)

    pltpu.make_async_copy(pgot, pgot, p_recv).wait()
    prompt_row = pair[...] + pgot[...]
    chip = ((y * nz + z) * nx + x) * 2
    toks = ny * rows
    lane = lax.broadcasted_iota(jnp.int32, (toks, 2 * voc), 1)
    entry = jnp.where(lane < voc, (chip + c) * voc + lane, (chip + 1 - c) * voc + lane - voc)
    lane_t = lax.broadcasted_iota(jnp.int32, (toks, LANES), 1)

    def slab(q):
        logits = acc[:, q].reshape(toks, 2 * voc)
        peak = jnp.max(logits, axis=1, keepdims=True)
        total = jnp.sum(jnp.exp(logits - peak), axis=1, keepdims=True)
        dig = abuf[:, q, ka].reshape(toks, LANES).astype(F32)
        want = (dig[:, 0:1] * 65536.0 + dig[:, 1:2] * 256.0 + dig[:, 2:3]).astype(jnp.int32)
        picked = jnp.sum(jnp.where(entry == want, logits, 0.0), axis=1, keepdims=True)
        side = jnp.where(lane_t == 0, peak, jnp.where(lane_t == 1, total, jnp.where(lane_t == 2, picked, 0.0)))
        if toks < LANES:
            side = jnp.concatenate([side, jnp.zeros((LANES - toks, LANES), F32)], axis=0)
        return jnp.where(row8 == 3, prompt_row, side.T[0:8, :])

    def step(i, carry):
        h = (i + 1) // 2
        d = nz // 2 + h * (1 - 2 * (i % 2))
        q = lax.rem(z + d, nz)
        tiles[i] = slab(q)
        pltpu.make_async_remote_copy(
            src_ref=tiles.at[i], dst_ref=got_z.at[i], send_sem=z_send.at[i], recv_sem=z_recv.at[i],
            device_id={AXZ: q}, device_id_type=MESH,
        ).start()
        return carry

    lax.fori_loop(0, nz - 1, step, 0)

    def merge(parts):
        top = functools.reduce(jnp.maximum, [p[0:1] for p in parts])
        out = sum(p * jnp.where(row8 == 1, jnp.exp(p[0:1] - top), 1.0) for p in parts)
        return jnp.where(row8 == 0, top, out)

    mine = slab(z)
    for i in range(nz - 1):
        pltpu.make_async_copy(got_z.at[i], got_z.at[i], z_recv.at[i]).wait()
    sum_y[...] = merge([mine] + [got_z[i] for i in range(nz - 1)])
    far = sorted(range(1, ny), key=lambda d: -hops(ny, d))
    for d in far:
        send(sum_y, got_y.at[d - 1], y_send.at[d - 1], y_recv.at[d - 1], {AXY: at(y, d, ny)})
    for d in reversed(far):
        pltpu.make_async_copy(got_y.at[d - 1], got_y.at[d - 1], y_recv.at[d - 1]).wait()
    sum_x[...] = merge([sum_y[...]] + [got_y[d - 1] for d in range(1, ny)])
    far = sorted(range(1, nx), key=lambda d: -hops(nx, d))
    for d in far:
        send(sum_x, got_x.at[d - 1], x_send.at[d - 1], x_recv.at[d - 1], {AXX: at(x, d, nx)})
    for d in reversed(far):
        pltpu.make_async_copy(got_x.at[d - 1], got_x.at[d - 1], x_recv.at[d - 1]).wait()
    done = merge([sum_x[...]] + [got_x[d - 1] for d in range(1, nx)])

    logprob = done[2:3] - (done[0:1] + jnp.log(done[1:2]))
    base = y * rows + x * 4
    r_out = lax.broadcasted_iota(jnp.int32, (2, 2), 0)
    w_out = lax.broadcasted_iota(jnp.int32, (2, 2), 1)
    value = jnp.zeros((2, 2), F32)
    for t in range(4):
        r, w = t // 2, t % 2
        one = jnp.sum(jnp.where(lane1 == base + t, logprob, 0.0), axis=1, keepdims=True)
        one = jnp.where(w < lens[r], one, 0.0)
        value = jnp.where((r_out == r) & (w_out == w), one, value)
    out1[...] = value
    moment = done[3:4] * (1.0 / GROUP)
    spot = lax.broadcasted_iota(jnp.int32, (1, 2), 1)
    adv = jnp.zeros((1, 2), F32)
    for r in range(2):
        mean = jnp.sum(jnp.where(lane1 == pids[r], moment, 0.0), axis=1, keepdims=True)
        square = jnp.sum(jnp.where(lane1 == pids[r] + PROMPTS, moment, 0.0), axis=1, keepdims=True)
        scale = jnp.sqrt(jnp.maximum(square - mean * mean, 1.0))
        adv = jnp.where(spot == r, (rewards[r] - mean) / scale, adv)
    out2[...] = adv

    for copy in started:
        copy.wait_send()
    for i in range(nz - 1):
        pltpu.make_async_copy(tiles.at[i], tiles.at[i], z_send.at[i]).wait()


def local(hidden, lm_head, reward_head, target_ids, lengths, prompt_ids):
    nx, ny, nz = (lax.axis_size(a) for a in (AXX, AXY, AXZ))
    width, voc = lm_head.shape
    tiles = width // LANES
    ka = tiles // 2
    kb = tiles - ka
    rows = nx * 4
    count_a = len(first_events(ny)) + len(second_events(ny, nz))
    count_b = len(first_events(nz)) + len(second_events(nz, ny))
    dma = pltpu.SemaphoreType.DMA
    vmem = pl.BlockSpec(memory_space=pltpu.VMEM)
    smem = pl.BlockSpec(memory_space=pltpu.SMEM)
    tile = (8, LANES)
    out1, out2 = pl.pallas_call(
        functools.partial(kernel, (nx, ny, nz, ka, kb)),
        out_shape=(jax.ShapeDtypeStruct((2, 2), F32), jax.ShapeDtypeStruct((1, 2), F32)),
        in_specs=[vmem, pl.BlockSpec(memory_space=pl.ANY), vmem, smem, smem, smem],
        out_specs=(vmem, vmem),
        scratch_shapes=[
            pltpu.VMEM((width, 2 * voc), jnp.bfloat16),
            pltpu.VMEM((ny, nz, ka + 1, rows, LANES), jnp.bfloat16),
            pltpu.VMEM((ny, nz, kb, rows, LANES), jnp.bfloat16),
            pltpu.VMEM((ny, nz, rows, 2 * voc), F32),
            pltpu.VMEM((nx, 2, 2, width), jnp.bfloat16),
            pltpu.VMEM((nx,) + tile, F32),
            pltpu.VMEM(tile, F32),
            pltpu.VMEM((nz - 1,) + tile, F32),
            pltpu.VMEM((nz - 1,) + tile, F32),
            pltpu.VMEM((ny - 1,) + tile, F32),
            pltpu.VMEM((nx - 1,) + tile, F32),
            pltpu.VMEM(tile, F32),
            pltpu.VMEM(tile, F32),
            pltpu.VMEM(tile, F32),
            pltpu.VMEM(tile, F32),
            dma, dma, dma,
            dma((nx - 1,)), dma((nx - 1,)), dma((nx - 1,)), dma((nx - 1,)),
            dma, dma,
            dma((count_a,)), dma((count_a,)), dma((count_b,)), dma((count_b,)),
            dma((nz - 1,)), dma((nz - 1,)), dma((ny - 1,)), dma((ny - 1,)), dma((nx - 1,)), dma((nx - 1,)),
        ],
        compiler_params=pltpu.CompilerParams(collective_id=0, has_side_effects=True),
        name="gather_score",
    )(hidden, lm_head, reward_head.reshape(1, width), target_ids, lengths, prompt_ids)
    return out1, out2.reshape(2)


def solution(mesh):
    split = Mesh(mesh.devices.reshape(mesh.shape["rep"], 8, 4, 2), REP_DP)
    placed = (P(REP_DP, None, None), P(None, REP_DP), P(), P(REP_DP, None), P(REP_DP), P(REP_DP))
    return jax.shard_map(
        local, mesh=split, in_specs=placed, out_specs=(P(REP_DP, None), P(REP_DP)), check_vma=False
    )
```

```python
import functools

import jax
import jax.numpy as jnp
from jax import lax
from jax.experimental import pallas as pl
from jax.experimental.pallas import tpu as pltpu
from jax.sharding import Mesh
from jax.sharding import PartitionSpec as P

GROUP = 16
PROMPTS = 64
REP_DP = ("rep", "dp_0", "dp_1", "dp_2")
AXY, AXZ, AXX, AXC = REP_DP
LANES = 128
MESH = pl.DeviceIdType.MESH
F32 = jnp.float32


def ring_offsets(n):
    order = [0]
    for d in range(1, n // 2 + 1):
        order.append(-d)
        if 2 * d < n:
            order.append(d)
    return order


def hops(n, off):
    return min(off % n, -off % n)


def first_events(n):
    out = []
    for d in range(1, n // 2 + 1):
        out.append((d, 1))
        if 2 * d < n:
            out.append((d, -1))
    return out


def second_events(n1, n2):
    out = []
    for j in range(n1):
        for d in range(1, n2 // 2 + 1):
            if 2 * d < n2:
                out.append((j, d, 1))
                out.append((j, d, -1))
            else:
                out.append((j, d, 1 if j % 2 == 0 else -1))
    return out


def groups_of(ny, nz):
    every = [(dy, dz) for dy in ring_offsets(ny) for dz in ring_offsets(nz)]
    return sorted(every, key=lambda g: hops(ny, g[0]) + hops(nz, g[1]))


def kernel(
    sizes, hid_in, whbm, rhead_in, ids_in, lens_in, pids_in, out1, out2,
    hid, rhead, ids, lens, pids,
    wmat, abuf, bbuf, cbuf, quarter, acc, side, gath, gmeta, meta, tiles, got_z, got_y, got_x, sum_y, sum_x, pair, pgot,
    in_sem, w_send, w_recv, g_send, g_recv, m_send, m_recv, p_send, p_recv,
    a_send, a_recv, b_send, b_recv, c_send, c_recv, z_send, z_recv, y_send, y_recv, x_send, x_recv,
):
    nx, ny, nz, ka, kb, kq = sizes
    rows = nx * 4
    voc = whbm.shape[1]
    y, z, x, c = (lax.axis_index(a) for a in (AXY, AXZ, AXX, AXC))

    def at(pos, off, n):
        return lax.rem(pos + (off % n), n)

    barrier = pltpu.get_barrier_semaphore()
    partners = [{AXX: at(x, d, nx)} for d in range(1, nx)]
    partners += [{AXY: at(y, d, ny)} for d in (1, -1)]
    partners += [{AXZ: at(z, d, nz)} for d in (1, -1)]
    partners += [{AXC: 1 - c}]
    for dev in partners:
        pl.semaphore_signal(barrier, inc=1, device_id=dev, device_id_type=MESH)

    loads = [
        pltpu.make_async_copy(src, dst, in_sem.at[i])
        for i, (src, dst) in enumerate((
            (hid_in, hid), (ids_in, ids), (lens_in, lens), (pids_in, pids), (rhead_in, rhead),
            (whbm, wmat.at[:, pl.ds(0, voc)]),
        ))
    ]
    for load in loads:
        load.start()
    loads[0].wait()
    loads[1].wait()

    row8 = lax.broadcasted_iota(jnp.int32, (8, LANES), 0)
    lane8 = lax.broadcasted_iota(jnp.int32, (8, LANES), 1)
    idv = jnp.zeros((8, LANES), jnp.int32)
    for t in range(4):
        idv = jnp.where(row8 == t, ids[t // 2, t % 2], idv)
    digits = jnp.where(lane8 == 0, idv >> 16, jnp.where(lane8 == 1, (idv >> 8) & 255, idv & 255))
    meta[...] = jnp.where(lane8 < 3, digits, 0).astype(F32)
    pl.semaphore_wait(barrier, len(partners))

    started = []

    def send(src, dst, ssem, rsem, dev, keep=True):
        copy = pltpu.make_async_remote_copy(
            src_ref=src, dst_ref=dst, send_sem=ssem, recv_sem=rsem, device_id=dev, device_id_type=MESH
        )
        copy.start()
        if keep:
            started.append(copy)

    def take(ref, sem):
        pltpu.make_async_copy(ref, ref, sem).wait()

    for d in range(1, nx):
        send(hid, gath.at[x], g_send.at[d - 1], g_recv.at[d - 1], {AXX: at(x, d, nx)})
    for d in range(1, nx):
        send(meta, gmeta.at[x], m_send.at[d - 1], m_recv.at[d - 1], {AXX: at(x, d, nx)})
    send(whbm, wmat.at[:, pl.ds(voc, voc)], w_send, w_recv, {AXC: 1 - c})

    gath[x] = hid[...]
    gmeta[x] = meta[...]

    for load in loads[2:5]:
        load.wait()
    rewards = []
    for r in range(2):
        both = sum(
            hid[r, :, pl.ds(k * LANES, LANES)].astype(F32) * rhead[k:k + 1].astype(F32)
            for k in range(rhead.shape[0])
        )
        both = jnp.sum(both, axis=1, keepdims=True)
        rewards.append(jnp.where(lens[r] == 1, both[0:1], both[1:2]))
    lane1 = lax.broadcasted_iota(jnp.int32, (1, LANES), 1)
    stacked = jnp.zeros((1, LANES), F32)
    for r in range(2):
        stacked += jnp.where(lane1 == pids[r], rewards[r], 0.0)
        stacked += jnp.where(lane1 == pids[r] + PROMPTS, rewards[r] * rewards[r], 0.0)
    pair[...] = jnp.where(row8 == 3, stacked, 0.0)

    for d in range(1, nx):
        src = at(x, -d, nx)
        take(gath.at[src], g_recv.at[d - 1])
        take(gmeta.at[src], m_recv.at[d - 1])

    whole = jnp.concatenate(
        [gath[i, r].astype(F32) for i in range(nx) for r in range(2)], axis=0
    ).astype(jnp.bfloat16)
    pieces = [whole[:, k * LANES:(k + 1) * LANES] for k in range(ka + kb + nx * kq)]
    for k in range(nx * kq):
        quarter[k // kq, k % kq] = pieces[ka + kb + k]
    for k in range(ka):
        abuf[y, z, k] = pieces[k]
    for k in range(kb):
        bbuf[y, z, k] = pieces[ka + k]
    abuf[y, z, ka] = jnp.concatenate([gmeta[i, 0:4] for i in range(nx)], axis=0).astype(jnp.bfloat16)
    for k in range(kq):
        abuf[y, z, ka + 1 + k] = quarter[x, k]

    send(pair, pgot, p_send, p_recv, {AXC: 1 - c})

    groups = groups_of(ny, nz)
    many = len(groups)
    place = {(dy % ny, dz % nz): i for i, (dy, dz) in enumerate(groups)}
    far_of = [hops(ny, dy) + hops(nz, dz) for dy, dz in groups]
    where = [(at(y, dy, ny), at(z, dz, nz)) for dy, dz in groups]

    def spread(i):
        for n, way in enumerate((1, -1)):
            send(
                abuf.at[where[i] + (pl.ds(ka + 1, kq),)], cbuf.at[(n,) + where[i]],
                c_send, c_recv.at[n * many + i], {AXX: at(x, way, nx)}, keep=False,
            )

    def spread_on(i):
        for n in range(2):
            take(cbuf.at[(n,) + where[i]], c_recv.at[n * many + i])
        n = i % 2
        send(
            cbuf.at[(n,) + where[i]], cbuf.at[(2,) + where[i]],
            c_send, c_recv.at[2 * many + i], {AXX: at(x, 1 - 2 * n, nx)}, keep=False,
        )

    def colour(buf, first, p1, n1, axis1, p2, n2, axis2, ssem, rsem):
        offs = ring_offsets(n1)
        ev1, ev2 = first_events(n1), second_events(n1, n2)
        index1 = {e: i for i, e in enumerate(ev1)}
        index2 = {e: len(ev1) + i for i, e in enumerate(ev2)}

        def block(off1, off2):
            i = place[(off1 % n1, off2 % n2) if first else (off2 % n2, off1 % n1)]
            return i, buf.at[where[i]]

        def put1(d, way):
            if (d, way) in index1:
                i = index1[(d, way)]
                b = block(-way * (d - 1), 0)[1]
                send(b, b, ssem.at[i], rsem.at[i], {axis1: at(p1, way, n1)})

        def put2(j, d, way):
            if (j, d, way) in index2:
                i = index2[(j, d, way)]
                b = block(offs[j], -way * (d - 1))[1]
                send(b, b, ssem.at[i], rsem.at[i], {axis2: at(p2, way, n2)})

        def begin():
            for way in (1, -1):
                put1(1, way)
            for way in (1, -1):
                put2(0, 1, way)
            if first:
                spread(0)

        def got1(d, way):
            i, b = block(-way * d, 0)
            take(b, rsem.at[index1[(d, way)]])
            put1(d + 1, way)
            j = [o % n1 for o in offs].index(-way * d % n1)
            for w2 in (1, -1):
                put2(j, 1, w2)
            if first:
                spread(i)

        def got2(j, d, way):
            i, b = block(offs[j], -way * d)
            take(b, rsem.at[index2[(j, d, way)]])
            put2(j, d + 1, way)
            if first:
                spread(i)

        events = [(e[0], 0, functools.partial(got1, *e)) for e in ev1]
        events += [
            (hops(n1, offs[e[0]]) + e[1], 1, functools.partial(got2, *e))
            for e in sorted(ev2, key=lambda e: (hops(n1, offs[e[0]]) + e[1], e[1], e[0]))
        ]
        return begin, events

    begin_a, events_a = colour(abuf, True, y, ny, AXY, z, nz, AXZ, a_send, a_recv)
    begin_b, events_b = colour(bbuf, False, z, nz, AXZ, y, ny, AXY, b_send, b_recv)
    begin_a()
    begin_b()

    wide = 2 * LANES
    chip = ((y * nz + z) * nx + x) * 2
    turns = [at(x, off, nx) for off in (0, -1, 1, 2)]
    starts = [pl.multiple_of((ka + kb + q * kq) * LANES, LANES) for q in turns]

    def product(chunk, last):
        def step(n, carry):
            cols = pl.ds(pl.multiple_of(n * wide, wide), wide)
            left = []
            for i in chunk:
                if last:
                    parts = [abuf[where[i] + (ka + 1 + k,)] for k in range(kq)]
                    parts += [cbuf[(r,) + where[i] + (k,)] for r in range(3) for k in range(kq)]
                else:
                    parts = [abuf[where[i] + (k,)] for k in range(ka)]
                    parts += [bbuf[where[i] + (k,)] for k in range(kb)]
                left.append(jnp.concatenate(parts, axis=1))
            left = jnp.concatenate(left, axis=0)
            if last:
                right = jnp.concatenate([wmat[pl.ds(s, kq * LANES), cols] for s in starts], axis=0)
            else:
                right = wmat[pl.ds(0, (ka + kb) * LANES), cols]
            part = jnp.dot(left, right, preferred_element_type=F32)
            for m, i in enumerate(chunk):
                piece = part[m * rows:(m + 1) * rows]
                if last:
                    piece = acc[where[i] + (slice(None), cols)] + piece
                acc[where[i] + (slice(None), cols)] = piece
            return carry

        lax.fori_loop(0, 2 * voc // wide, step, 0)

    def score(chunk):
        toks = len(chunk) * rows

        def logits():
            return jnp.concatenate([acc[where[i]] for i in chunk], axis=0)

        lane = lax.broadcasted_iota(jnp.int32, (toks, 2 * voc), 1)
        entry = jnp.where(lane < voc, (chip + c) * voc + lane, (chip + 1 - c) * voc + lane - voc)
        lane_t = lax.broadcasted_iota(jnp.int32, (toks, LANES), 1)
        peak = jnp.max(logits(), axis=1, keepdims=True)
        total = jnp.sum(jnp.exp(logits() - peak), axis=1, keepdims=True)
        dig = jnp.concatenate([abuf[where[i] + (ka,)] for i in chunk], axis=0).astype(F32)
        want = (dig[:, 0:1] * 65536.0 + dig[:, 1:2] * 256.0 + dig[:, 2:3]).astype(jnp.int32)
        picked = jnp.sum(jnp.where(entry == want, logits(), 0.0), axis=1, keepdims=True)
        out = jnp.where(lane_t == 0, peak, jnp.where(lane_t == 1, total, jnp.where(lane_t == 2, picked, 0.0)))
        for m, i in enumerate(chunk):
            side[where[i][1], where[i][0]] = out[m * rows:(m + 1) * rows]

    cuts = [0, many // 4, many // 2, 3 * many // 4, 7 * many // 8, many]
    chunks = [list(range(s, e)) for s, e in zip(cuts[:-1], cuts[1:])]
    whole_part, last_part = list(chunks), list(chunks)
    spread_wait = list(range(many))
    waves = ny // 2 + nz // 2
    ready = False
    for wave in range(1, waves + 3):
        for kind in (0, 1):
            mine = [[e for e in ev if e[0] == wave and e[1] == kind] for ev in (events_a, events_b)]
            for n in range(max(len(m) for m in mine)):
                for m in mine:
                    if n < len(m):
                        m[n][2]()
        for i in [i for i in spread_wait if far_of[i] < wave]:
            spread_on(i)
            spread_wait.remove(i)
        while whole_part and max(far_of[i] for i in whole_part[0]) <= wave:
            if not ready:
                loads[5].wait()
                take(wmat.at[:, pl.ds(voc, voc)], w_recv)
                ready = True
            product(whole_part.pop(0), False)
        while last_part and max(far_of[i] for i in last_part[0]) <= wave - 2:
            chunk = last_part.pop(0)
            for i in chunk:
                take(cbuf.at[(2,) + where[i]], c_recv.at[2 * many + i])
            product(chunk, True)
            score(chunk)

    take(pgot, p_recv)
    prompt_row = pair[...] + pgot[...]

    def slab(q):
        block = side[q].reshape(ny * rows, LANES)
        if ny * rows < LANES:
            block = jnp.concatenate([block, jnp.zeros((LANES - ny * rows, LANES), F32)], axis=0)
        return jnp.where(row8 == 3, prompt_row, block.T[0:8, :])

    def step(i, carry):
        h = (i + 1) // 2
        d = nz // 2 + h * (1 - 2 * (i % 2))
        q = lax.rem(z + d, nz)
        tiles[i] = slab(q)
        pltpu.make_async_remote_copy(
            src_ref=tiles.at[i], dst_ref=got_z.at[i], send_sem=z_send.at[i], recv_sem=z_recv.at[i],
            device_id={AXZ: q}, device_id_type=MESH,
        ).start()
        return carry

    lax.fori_loop(0, nz - 1, step, 0)

    def merge(parts):
        top = functools.reduce(jnp.maximum, [p[0:1] for p in parts])
        out = sum(p * jnp.where(row8 == 1, jnp.exp(p[0:1] - top), 1.0) for p in parts)
        return jnp.where(row8 == 0, top, out)

    mine = slab(z)
    for i in range(nz - 1):
        pltpu.make_async_copy(got_z.at[i], got_z.at[i], z_recv.at[i]).wait()
    sum_y[...] = merge([mine] + [got_z[i] for i in range(nz - 1)])
    far = sorted(range(1, ny), key=lambda d: -hops(ny, d))
    for d in far:
        send(sum_y, got_y.at[d - 1], y_send.at[d - 1], y_recv.at[d - 1], {AXY: at(y, d, ny)})
    for d in reversed(far):
        pltpu.make_async_copy(got_y.at[d - 1], got_y.at[d - 1], y_recv.at[d - 1]).wait()
    sum_x[...] = merge([sum_y[...]] + [got_y[d - 1] for d in range(1, ny)])
    far = sorted(range(1, nx), key=lambda d: -hops(nx, d))
    for d in far:
        send(sum_x, got_x.at[d - 1], x_send.at[d - 1], x_recv.at[d - 1], {AXX: at(x, d, nx)})
    for d in reversed(far):
        pltpu.make_async_copy(got_x.at[d - 1], got_x.at[d - 1], x_recv.at[d - 1]).wait()
    done = merge([sum_x[...]] + [got_x[d - 1] for d in range(1, nx)])

    logprob = done[2:3] - (done[0:1] + jnp.log(done[1:2]))
    base = y * rows + x * 4
    r_out = lax.broadcasted_iota(jnp.int32, (2, 2), 0)
    w_out = lax.broadcasted_iota(jnp.int32, (2, 2), 1)
    value = jnp.zeros((2, 2), F32)
    for t in range(4):
        r, w = t // 2, t % 2
        one = jnp.sum(jnp.where(lane1 == base + t, logprob, 0.0), axis=1, keepdims=True)
        one = jnp.where(w < lens[r], one, 0.0)
        value = jnp.where((r_out == r) & (w_out == w), one, value)
    out1[...] = value
    moment = done[3:4] * (1.0 / GROUP)
    spot = lax.broadcasted_iota(jnp.int32, (1, 2), 1)
    adv = jnp.zeros((1, 2), F32)
    for r in range(2):
        mean = jnp.sum(jnp.where(lane1 == pids[r], moment, 0.0), axis=1, keepdims=True)
        square = jnp.sum(jnp.where(lane1 == pids[r] + PROMPTS, moment, 0.0), axis=1, keepdims=True)
        scale = jnp.sqrt(jnp.maximum(square - mean * mean, 1.0))
        adv = jnp.where(spot == r, (rewards[r] - mean) / scale, adv)
    out2[...] = adv

    for copy in started:
        copy.wait_send()
    take(cbuf, c_send)
    for i in range(nz - 1):
        pltpu.make_async_copy(tiles.at[i], tiles.at[i], z_send.at[i]).wait()


def local(hidden, lm_head, reward_head, target_ids, lengths, prompt_ids):
    nx, ny, nz = (lax.axis_size(a) for a in (AXX, AXY, AXZ))
    width, voc = lm_head.shape
    tiles = width // LANES
    kq = max(1, tiles * 3 // (7 * nx))
    ka = (tiles - kq * nx) * 3 // 8
    kb = tiles - kq * nx - ka
    rows = nx * 4
    count_a = len(first_events(ny)) + len(second_events(ny, nz))
    count_b = len(first_events(nz)) + len(second_events(nz, ny))
    dma = pltpu.SemaphoreType.DMA
    vmem = pl.BlockSpec(memory_space=pltpu.VMEM)
    tile = (8, LANES)
    out1, out2 = pl.pallas_call(
        functools.partial(kernel, (nx, ny, nz, ka, kb, kq)),
        out_shape=(jax.ShapeDtypeStruct((2, 2), F32), jax.ShapeDtypeStruct((1, 2), F32)),
        in_specs=[pl.BlockSpec(memory_space=pl.ANY)] * 6,
        out_specs=(vmem, vmem),
        scratch_shapes=[
            pltpu.VMEM((2, 2, width), jnp.bfloat16),
            pltpu.VMEM((tiles, LANES), jnp.bfloat16),
            pltpu.SMEM((2, 2), jnp.int32),
            pltpu.SMEM((2,), jnp.int32),
            pltpu.SMEM((2,), jnp.int32),
            pltpu.VMEM((width, 2 * voc), jnp.bfloat16),
            pltpu.VMEM((ny, nz, ka + 1 + kq, rows, LANES), jnp.bfloat16),
            pltpu.VMEM((ny, nz, kb, rows, LANES), jnp.bfloat16),
            pltpu.VMEM((3, ny, nz, kq, rows, LANES), jnp.bfloat16),
            pltpu.VMEM((nx, kq, rows, LANES), jnp.bfloat16),
            pltpu.VMEM((ny, nz, rows, 2 * voc), F32),
            pltpu.VMEM((nz, ny, rows, LANES), F32),
            pltpu.VMEM((nx, 2, 2, width), jnp.bfloat16),
            pltpu.VMEM((nx,) + tile, F32),
            pltpu.VMEM(tile, F32),
            pltpu.VMEM((nz - 1,) + tile, F32),
            pltpu.VMEM((nz - 1,) + tile, F32),
            pltpu.VMEM((ny - 1,) + tile, F32),
            pltpu.VMEM((nx - 1,) + tile, F32),
            pltpu.VMEM(tile, F32),
            pltpu.VMEM(tile, F32),
            pltpu.VMEM(tile, F32),
            pltpu.VMEM(tile, F32),
            dma((6,)), dma, dma,
            dma((nx - 1,)), dma((nx - 1,)), dma((nx - 1,)), dma((nx - 1,)),
            dma, dma,
            dma((count_a,)), dma((count_a,)), dma((count_b,)), dma((count_b,)),
            dma, dma((3 * ny * nz,)),
            dma((nz - 1,)), dma((nz - 1,)), dma((ny - 1,)), dma((ny - 1,)), dma((nx - 1,)), dma((nx - 1,)),
        ],
        compiler_params=pltpu.CompilerParams(collective_id=0, has_side_effects=True),
        name="gather_score",
    )(hidden, lm_head, reward_head.reshape(tiles, LANES), target_ids, lengths, prompt_ids)
    return out1, out2.reshape(2)


def solution(mesh):
    split = Mesh(mesh.devices.reshape(mesh.shape["rep"], 8, 4, 2), REP_DP)
    placed = (P(REP_DP, None, None), P(None, REP_DP), P(), P(REP_DP, None), P(REP_DP), P(REP_DP))
    return jax.shard_map(
        local, mesh=split, in_specs=placed, out_specs=(P(REP_DP, None), P(REP_DP)), check_vma=False
    )
```

```python
import functools

import jax
import jax.numpy as jnp
from jax import lax
from jax.experimental import pallas as pl
from jax.experimental.pallas import tpu as pltpu
from jax.sharding import Mesh
from jax.sharding import PartitionSpec as P

GROUP = 16
PROMPTS = 64
REP_DP = ("rep", "dp_0", "dp_1", "dp_2")
AXY, AXZ, AXX, AXC = REP_DP
LANES = 128
MESH = pl.DeviceIdType.MESH
F32 = jnp.float32


def ring_offsets(n):
    order = [0]
    for d in range(1, n // 2 + 1):
        order.append(-d)
        if 2 * d < n:
            order.append(d)
    return order


def hops(n, off):
    return min(off % n, -off % n)


def first_events(n):
    out = []
    for d in range(1, n // 2 + 1):
        out.append((d, 1))
        if 2 * d < n:
            out.append((d, -1))
    return out


def second_events(n1, n2):
    out = []
    for j in range(n1):
        for d in range(1, n2 // 2 + 1):
            if 2 * d < n2:
                out.append((j, d, 1))
                out.append((j, d, -1))
            else:
                out.append((j, d, 1 if j % 2 == 0 else -1))
    return out


def groups_of(ny, nz):
    every = [(dy, dz) for dy in ring_offsets(ny) for dz in ring_offsets(nz)]
    return sorted(every, key=lambda g: hops(ny, g[0]) + hops(nz, g[1]))


def kernel(
    sizes, hid_in, whbm, rhead_in, ids_in, lens_in, pids_in, out1, out2,
    hid, rhead, ids, lens, pids,
    wmat, abuf, bbuf, cbuf, quarter, acc, side, gath, gmeta, meta, tiles, got_z, got_y, got_x, sum_y, sum_x, pair, pgot,
    in_sem, w_send, w_recv, g_send, g_recv, m_send, m_recv, p_send, p_recv,
    a_send, a_recv, b_send, b_recv, c_send, c_recv, d_recv, z_send, z_recv, y_send, y_recv, x_send, x_recv,
):
    nx, ny, nz, ka, kb, kq = sizes
    rows = nx * 4
    voc = whbm.shape[1]
    y, z, x, c = (lax.axis_index(a) for a in (AXY, AXZ, AXX, AXC))

    def at(pos, off, n):
        return lax.rem(pos + (off % n), n)

    barrier = pltpu.get_barrier_semaphore()
    partners = [{AXX: at(x, d, nx)} for d in range(1, nx)]
    partners += [{AXY: at(y, d, ny)} for d in (1, -1)]
    partners += [{AXZ: at(z, d, nz)} for d in (1, -1)]
    partners += [{AXC: 1 - c}]
    for dev in partners:
        pl.semaphore_signal(barrier, inc=1, device_id=dev, device_id_type=MESH)

    loads = [
        pltpu.make_async_copy(src, dst, in_sem.at[i])
        for i, (src, dst) in enumerate((
            (hid_in, hid), (ids_in, ids), (lens_in, lens), (pids_in, pids), (rhead_in, rhead),
            (whbm, wmat.at[:, pl.ds(0, voc)]),
        ))
    ]
    for load in loads:
        load.start()
    loads[0].wait()
    loads[1].wait()

    row8 = lax.broadcasted_iota(jnp.int32, (8, LANES), 0)
    lane8 = lax.broadcasted_iota(jnp.int32, (8, LANES), 1)
    idv = jnp.zeros((8, LANES), jnp.int32)
    for t in range(4):
        idv = jnp.where(row8 == t, ids[t // 2, t % 2], idv)
    digits = jnp.where(lane8 == 0, idv >> 16, jnp.where(lane8 == 1, (idv >> 8) & 255, idv & 255))
    meta[...] = jnp.where(lane8 < 3, digits, 0).astype(F32)
    pl.semaphore_wait(barrier, len(partners))

    started = []

    def send(src, dst, ssem, rsem, dev, keep=True):
        copy = pltpu.make_async_remote_copy(
            src_ref=src, dst_ref=dst, send_sem=ssem, recv_sem=rsem, device_id=dev, device_id_type=MESH
        )
        copy.start()
        if keep:
            started.append(copy)

    def take(ref, sem):
        pltpu.make_async_copy(ref, ref, sem).wait()

    def take_tiles(n, sem):
        take(bbuf.at[pl.ds(0, n)], sem)

    for d in range(1, nx):
        send(hid, gath.at[x], g_send.at[d - 1], g_recv.at[d - 1], {AXX: at(x, d, nx)})
    for d in range(1, nx):
        send(meta, gmeta.at[x], m_send, m_recv.at[d - 1], {AXX: at(x, d, nx)}, keep=False)
    send(whbm, wmat.at[:, pl.ds(voc, voc)], w_send, w_recv, {AXC: 1 - c})

    gath[x] = hid[...]
    gmeta[x] = meta[...]

    for load in loads[2:5]:
        load.wait()
    rewards = []
    for r in range(2):
        both = sum(
            hid[r, :, pl.ds(k * LANES, LANES)].astype(F32) * rhead[k:k + 1].astype(F32)
            for k in range(rhead.shape[0])
        )
        both = jnp.sum(both, axis=1, keepdims=True)
        rewards.append(jnp.where(lens[r] == 1, both[0:1], both[1:2]))
    lane1 = lax.broadcasted_iota(jnp.int32, (1, LANES), 1)
    stacked = jnp.zeros((1, LANES), F32)
    for r in range(2):
        stacked += jnp.where(lane1 == pids[r], rewards[r], 0.0)
        stacked += jnp.where(lane1 == pids[r] + PROMPTS, rewards[r] * rewards[r], 0.0)
    pair[...] = jnp.where(row8 == 3, stacked, 0.0)

    for d in range(1, nx):
        src = at(x, -d, nx)
        take(gath.at[src], g_recv.at[d - 1])
        take(gmeta.at[src], m_recv.at[d - 1])

    whole = jnp.concatenate(
        [gath[i, r].astype(F32) for i in range(nx) for r in range(2)], axis=0
    ).astype(jnp.bfloat16)
    pieces = [whole[:, k * LANES:(k + 1) * LANES] for k in range(ka + kb + nx * kq)]
    for k in range(nx * kq):
        quarter[k // kq, k % kq] = pieces[ka + kb + k]
    base_a, base_b = (y * nz + z) * (ka + 1 + kq), (y * nz + z) * kb
    for k in range(ka):
        abuf[base_a + k] = pieces[k]
    for k in range(kb):
        bbuf[base_b + k] = pieces[ka + k]
    abuf[base_a + ka] = jnp.concatenate([gmeta[i, 0:4] for i in range(nx)], axis=0).astype(jnp.bfloat16)
    for k in range(kq):
        abuf[base_a + ka + 1 + k] = quarter[x, k]

    send(pair, pgot, p_send, p_recv, {AXC: 1 - c})

    groups = groups_of(ny, nz)
    many = len(groups)
    place = {(dy % ny, dz % nz): i for i, (dy, dz) in enumerate(groups)}
    far_of = [hops(ny, dy) + hops(nz, dz) for dy, dz in groups]
    where = [(at(y, dy, ny), at(z, dz, nz)) for dy, dz in groups]
    flat = [qy * nz + qz for qy, qz in where]

    def in_a(i, k=0):
        return flat[i] * (ka + 1 + kq) + k

    def in_b(i, k=0):
        return flat[i] * kb + k

    def in_c(r, i, k=0):
        return (r * many + flat[i]) * kq + k

    def block_c(r, i):
        return cbuf.at[pl.ds(in_c(r, i), kq)]

    wave_of = [[i for i in range(many) if far_of[i] == w] for w in range(ny // 2 + nz // 2 + 1)]

    chunks = [sum(wave_of[:3], [])] + wave_of[3:-2] + [sum(wave_of[-2:], [])]
    part_of = {i: n for n, chunk in enumerate(chunks) for i in chunk}

    def spread(i):
        for n, way in enumerate((1, -1)):
            send(
                abuf.at[pl.ds(in_a(i, ka + 1), kq)], block_c(n, i),
                c_send, c_recv.at[2 * far_of[i] + n], {AXX: at(x, way, nx)}, keep=False,
            )

    def spread_on(wave):
        for n in range(2):
            take_tiles(len(wave_of[wave]) * kq, c_recv.at[2 * wave + n])
        for i in wave_of[wave]:
            n = i % 2
            send(
                block_c(n, i), block_c(2, i),
                c_send, d_recv.at[part_of[i]], {AXX: at(x, 1 - 2 * n, nx)}, keep=False,
            )

    def colour(first, p1, n1, axis1, p2, n2, axis2, ssem, rsem):
        offs = ring_offsets(n1)
        ev1, ev2 = first_events(n1), second_events(n1, n2)
        index1 = {e: i for i, e in enumerate(ev1)}
        index2 = {e: len(ev1) + i for i, e in enumerate(ev2)}

        def block(off1, off2):
            i = place[(off1 % n1, off2 % n2) if first else (off2 % n2, off1 % n1)]
            return i, (abuf.at[pl.ds(in_a(i), ka + 1 + kq)] if first else bbuf.at[pl.ds(in_b(i), kb)])

        def put1(d, way):
            if (d, way) in index1:
                i = index1[(d, way)]
                b = block(-way * (d - 1), 0)[1]
                send(b, b, ssem, rsem.at[i], {axis1: at(p1, way, n1)}, keep=False)

        def put2(j, d, way):
            if (j, d, way) in index2:
                i = index2[(j, d, way)]
                b = block(offs[j], -way * (d - 1))[1]
                send(b, b, ssem, rsem.at[i], {axis2: at(p2, way, n2)}, keep=False)

        def begin():
            for way in (1, -1):
                put1(1, way)
            for way in (1, -1):
                put2(0, 1, way)
            if first:
                spread(0)

        def got1(d, way):
            i, b = block(-way * d, 0)
            take(b, rsem.at[index1[(d, way)]])
            put1(d + 1, way)
            j = [o % n1 for o in offs].index(-way * d % n1)
            for w2 in (1, -1):
                put2(j, 1, w2)
            if first:
                spread(i)

        def got2(j, d, way):
            i, b = block(offs[j], -way * d)
            take(b, rsem.at[index2[(j, d, way)]])
            put2(j, d + 1, way)
            if first:
                spread(i)

        events = [(e[0], 0, functools.partial(got1, *e)) for e in ev1]
        events += [
            (hops(n1, offs[e[0]]) + e[1], 1, functools.partial(got2, *e))
            for e in sorted(ev2, key=lambda e: (hops(n1, offs[e[0]]) + e[1], e[1], e[0]))
        ]
        return begin, events

    begin_a, events_a = colour(True, y, ny, AXY, z, nz, AXZ, a_send, a_recv)
    begin_b, events_b = colour(False, z, nz, AXZ, y, ny, AXY, b_send, b_recv)
    begin_a()
    begin_b()

    wide = 2 * LANES
    chip = ((y * nz + z) * nx + x) * 2
    turns = [at(x, off, nx) for off in (0, -1, 1, 2)]
    starts = [pl.multiple_of((ka + kb + q * kq) * LANES, LANES) for q in turns]

    def product(chunk, last):
        def step(n, carry):
            cols = pl.ds(pl.multiple_of(n * wide, wide), wide)
            left = []
            for i in chunk:
                if last:
                    parts = [abuf[in_a(i, ka + 1 + k)] for k in range(kq)]
                    parts += [cbuf[in_c(r, i, k)] for r in range(3) for k in range(kq)]
                else:
                    parts = [abuf[in_a(i, k)] for k in range(ka)]
                    parts += [bbuf[in_b(i, k)] for k in range(kb)]
                left.append(jnp.concatenate(parts, axis=1))
            left = jnp.concatenate(left, axis=0)
            if last:
                right = jnp.concatenate([wmat[pl.ds(s, kq * LANES), cols] for s in starts], axis=0)
            else:
                right = wmat[pl.ds(0, (ka + kb) * LANES), cols]
            part = jnp.dot(left, right, preferred_element_type=F32)
            for m, i in enumerate(chunk):
                piece = part[m * rows:(m + 1) * rows]
                if last:
                    piece = acc[where[i] + (slice(None), cols)] + piece
                acc[where[i] + (slice(None), cols)] = piece
            return carry

        lax.fori_loop(0, 2 * voc // wide, step, 0)

    def score(chunk):
        toks = len(chunk) * rows

        def logits():
            return jnp.concatenate([acc[where[i]] for i in chunk], axis=0)

        lane = lax.broadcasted_iota(jnp.int32, (toks, 2 * voc), 1)
        entry = jnp.where(lane < voc, (chip + c) * voc + lane, (chip + 1 - c) * voc + lane - voc)
        lane_t = lax.broadcasted_iota(jnp.int32, (toks, LANES), 1)
        peak = jnp.max(logits(), axis=1, keepdims=True)
        total = jnp.sum(jnp.exp(logits() - peak), axis=1, keepdims=True)
        dig = jnp.concatenate([abuf[in_a(i, ka)] for i in chunk], axis=0).astype(F32)
        want = (dig[:, 0:1] * 65536.0 + dig[:, 1:2] * 256.0 + dig[:, 2:3]).astype(jnp.int32)
        picked = jnp.sum(jnp.where(entry == want, logits(), 0.0), axis=1, keepdims=True)
        out = jnp.where(lane_t == 0, peak, jnp.where(lane_t == 1, total, jnp.where(lane_t == 2, picked, 0.0)))
        for m, i in enumerate(chunk):
            side[where[i][1], where[i][0]] = out[m * rows:(m + 1) * rows]

    whole_part, last_part = list(chunks), list(enumerate(chunks))
    waves = ny // 2 + nz // 2
    ready = False
    for wave in range(1, waves + 3):
        for kind in (0, 1):
            mine = [[e for e in ev if e[0] == wave and e[1] == kind] for ev in (events_a, events_b)]
            for n in range(max(len(m) for m in mine)):
                for m in mine:
                    if n < len(m):
                        m[n][2]()
        if wave - 1 <= waves:
            spread_on(wave - 1)
        while whole_part and max(far_of[i] for i in whole_part[0]) <= wave:
            if not ready:
                loads[5].wait()
                take(wmat.at[:, pl.ds(voc, voc)], w_recv)
                ready = True
            product(whole_part.pop(0), False)
        while last_part and max(far_of[i] for i in last_part[0][1]) <= wave - 2:
            part, chunk = last_part.pop(0)
            take_tiles(len(chunk) * kq, d_recv.at[part])
            product(chunk, True)
            score(chunk)

    take(pgot, p_recv)
    prompt_row = pair[...] + pgot[...]

    def slab(q):
        block = side[q].reshape(ny * rows, LANES)
        if ny * rows < LANES:
            block = jnp.concatenate([block, jnp.zeros((LANES - ny * rows, LANES), F32)], axis=0)
        return jnp.where(row8 == 3, prompt_row, block.T[0:8, :])

    def step(i, carry):
        h = (i + 1) // 2
        d = nz // 2 + h * (1 - 2 * (i % 2))
        q = lax.rem(z + d, nz)
        tiles[i] = slab(q)
        pltpu.make_async_remote_copy(
            src_ref=tiles.at[i], dst_ref=got_z.at[i], send_sem=z_send, recv_sem=z_recv.at[i],
            device_id={AXZ: q}, device_id_type=MESH,
        ).start()
        return carry

    lax.fori_loop(0, nz - 1, step, 0)

    def merge(parts):
        top = functools.reduce(jnp.maximum, [p[0:1] for p in parts])
        out = sum(p * jnp.where(row8 == 1, jnp.exp(p[0:1] - top), 1.0) for p in parts)
        return jnp.where(row8 == 0, top, out)

    mine = slab(z)
    for i in range(nz - 1):
        pltpu.make_async_copy(got_z.at[i], got_z.at[i], z_recv.at[i]).wait()
    sum_y[...] = merge([mine] + [got_z[i] for i in range(nz - 1)])
    far = sorted(range(1, ny), key=lambda d: -hops(ny, d))
    for d in far:
        send(sum_y, got_y.at[d - 1], y_send, y_recv.at[d - 1], {AXY: at(y, d, ny)}, keep=False)
    for d in reversed(far):
        pltpu.make_async_copy(got_y.at[d - 1], got_y.at[d - 1], y_recv.at[d - 1]).wait()
    sum_x[...] = merge([sum_y[...]] + [got_y[d - 1] for d in range(1, ny)])
    far = sorted(range(1, nx), key=lambda d: -hops(nx, d))
    for d in far:
        send(sum_x, got_x.at[d - 1], x_send, x_recv.at[d - 1], {AXX: at(x, d, nx)}, keep=False)
    for d in reversed(far):
        pltpu.make_async_copy(got_x.at[d - 1], got_x.at[d - 1], x_recv.at[d - 1]).wait()
    done = merge([sum_x[...]] + [got_x[d - 1] for d in range(1, nx)])

    logprob = done[2:3] - (done[0:1] + jnp.log(done[1:2]))
    base = y * rows + x * 4
    r_out = lax.broadcasted_iota(jnp.int32, (2, 2), 0)
    w_out = lax.broadcasted_iota(jnp.int32, (2, 2), 1)
    value = jnp.zeros((2, 2), F32)
    for t in range(4):
        r, w = t // 2, t % 2
        one = jnp.sum(jnp.where(lane1 == base + t, logprob, 0.0), axis=1, keepdims=True)
        one = jnp.where(w < lens[r], one, 0.0)
        value = jnp.where((r_out == r) & (w_out == w), one, value)
    out1[...] = value
    moment = done[3:4] * (1.0 / GROUP)
    spot = lax.broadcasted_iota(jnp.int32, (1, 2), 1)
    adv = jnp.zeros((1, 2), F32)
    for r in range(2):
        mean = jnp.sum(jnp.where(lane1 == pids[r], moment, 0.0), axis=1, keepdims=True)
        square = jnp.sum(jnp.where(lane1 == pids[r] + PROMPTS, moment, 0.0), axis=1, keepdims=True)
        scale = jnp.sqrt(jnp.maximum(square - mean * mean, 1.0))
        adv = jnp.where(spot == r, (rewards[r] - mean) / scale, adv)
    out2[...] = adv

    for copy in started:
        copy.wait_send()
    take_tiles((many - 1) * (ka + 1 + kq), a_send)
    take_tiles((many - 1) * kb, b_send)
    take_tiles(3 * many * kq, c_send)
    for n, sem in ((nz - 1, z_send), (ny - 1, y_send), (nx - 1, x_send), (nx - 1, m_send)):
        take_tiles(n, sem)


def local(hidden, lm_head, reward_head, target_ids, lengths, prompt_ids):
    nx, ny, nz = (lax.axis_size(a) for a in (AXX, AXY, AXZ))
    width, voc = lm_head.shape
    tiles = width // LANES
    kq = max(1, tiles * 3 // (7 * nx))
    ka = (tiles - kq * nx) * 3 // 8
    kb = tiles - kq * nx - ka
    rows = nx * 4
    count_a = len(first_events(ny)) + len(second_events(ny, nz))
    count_b = len(first_events(nz)) + len(second_events(nz, ny))
    dma = pltpu.SemaphoreType.DMA
    vmem = pl.BlockSpec(memory_space=pltpu.VMEM)
    tile = (8, LANES)
    out1, out2 = pl.pallas_call(
        functools.partial(kernel, (nx, ny, nz, ka, kb, kq)),
        out_shape=(jax.ShapeDtypeStruct((2, 2), F32), jax.ShapeDtypeStruct((1, 2), F32)),
        in_specs=[pl.BlockSpec(memory_space=pl.ANY)] * 6,
        out_specs=(vmem, vmem),
        scratch_shapes=[
            pltpu.VMEM((2, 2, width), jnp.bfloat16),
            pltpu.VMEM((tiles, LANES), jnp.bfloat16),
            pltpu.SMEM((2, 2), jnp.int32),
            pltpu.SMEM((2,), jnp.int32),
            pltpu.SMEM((2,), jnp.int32),
            pltpu.VMEM((width, 2 * voc), jnp.bfloat16),
            pltpu.VMEM((ny * nz * (ka + 1 + kq), rows, LANES), jnp.bfloat16),
            pltpu.VMEM((ny * nz * kb, rows, LANES), jnp.bfloat16),
            pltpu.VMEM((3 * ny * nz * kq, rows, LANES), jnp.bfloat16),
            pltpu.VMEM((nx, kq, rows, LANES), jnp.bfloat16),
            pltpu.VMEM((ny, nz, rows, 2 * voc), F32),
            pltpu.VMEM((nz, ny, rows, LANES), F32),
            pltpu.VMEM((nx, 2, 2, width), jnp.bfloat16),
            pltpu.VMEM((nx,) + tile, F32),
            pltpu.VMEM(tile, F32),
            pltpu.VMEM((nz - 1,) + tile, F32),
            pltpu.VMEM((nz - 1,) + tile, F32),
            pltpu.VMEM((ny - 1,) + tile, F32),
            pltpu.VMEM((nx - 1,) + tile, F32),
            pltpu.VMEM(tile, F32),
            pltpu.VMEM(tile, F32),
            pltpu.VMEM(tile, F32),
            pltpu.VMEM(tile, F32),
            dma((6,)), dma, dma,
            dma((nx - 1,)), dma((nx - 1,)), dma, dma((nx - 1,)),
            dma, dma,
            dma, dma((count_a,)), dma, dma((count_b,)),
            dma, dma((ny + nz + 2,)), dma((ny // 2 + nz // 2 - 2,)),
            dma, dma((nz - 1,)), dma, dma((ny - 1,)), dma, dma((nx - 1,)),
        ],
        compiler_params=pltpu.CompilerParams(collective_id=0, has_side_effects=True),
        name="gather_score",
    )(hidden, lm_head, reward_head.reshape(tiles, LANES), target_ids, lengths, prompt_ids)
    return out1, out2.reshape(2)


def solution(mesh):
    split = Mesh(mesh.devices.reshape(mesh.shape["rep"], 8, 4, 2), REP_DP)
    placed = (P(REP_DP, None, None), P(None, REP_DP), P(), P(REP_DP, None), P(REP_DP), P(REP_DP))
    return jax.shard_map(
        local, mesh=split, in_specs=placed, out_specs=(P(REP_DP, None), P(REP_DP)), check_vma=False
    )
```

```python
import functools

import jax
import jax.numpy as jnp
from jax import lax
from jax.experimental import pallas as pl
from jax.experimental.pallas import tpu as pltpu
from jax.sharding import Mesh
from jax.sharding import PartitionSpec as P

GROUP = 16
PROMPTS = 64
REP_DP = ("rep", "dp_0", "dp_1", "dp_2")
AXY, AXZ, AXX, AXC = REP_DP
LANES = 128
MESH = pl.DeviceIdType.MESH
F32 = jnp.float32


def ring_offsets(n):
    order = [0]
    for d in range(1, n // 2 + 1):
        order.append(-d)
        if 2 * d < n:
            order.append(d)
    return order


def hops(n, off):
    return min(off % n, -off % n)


def plan(ny, nz, sizes, depth=1.5, rate=46.6e3, lag=2.2, least=8, most=16):
    parts = {"a": (0, ny, nz), "b": (1, nz, ny), "c": (0, ny, nz)}
    groups = [(dy % ny, dz % nz) for dy in ring_offsets(ny) for dz in ring_offsets(nz)]
    now, free, pending, issued, arrive = [0.0], {}, {}, {}, {}
    ops = []
    extra = {"a": 0, "b": 0, "c": 2}

    def queue(link, left, colour, event, what):
        pending.setdefault(link, []).append((-left, len(ops), colour, event, what))

    def issue():
        for link, wait in sorted(pending.items()):
            while wait and free.get(link, 0.0) - now[0] < depth:
                wait.sort(key=lambda w: w[0])
                left, _, colour, event, what = wait.pop(0)
                start = max(now[0], free.get(link, 0.0))
                free[link] = start + sizes[colour] / rate
                arrive[event] = max(arrive.get(event, 0.0), free[link] + lag)
                issued[event] = issued.get(event, 0) + 1
                ops.append(("send", link, event, what))

    def place(colour, off1, off2):
        swap, n1, n2 = parts[colour]
        return (off2 % n2, off1 % n1) if swap else (off1 % n1, off2 % n2)

    def ways(n, d):
        return (1, -1) if 2 * d < n else (1,)

    need, outstanding = {}, set()

    def put1(colour, d, way):
        swap, n1, n2 = parts[colour]
        if d <= n1 // 2 and way in ways(n1, d):
            event = ("p1", colour, d)
            need[event] = len(ways(n1, d))
            outstanding.add(event)
            queue(("zy" if swap else "yz")[0] + "+-"[way < 0], n1 // 2 - d + n2 // 2 + extra[colour], colour, event,
                  place(colour, -way * (d - 1), 0))

    def put2(colour, j, d, way):
        swap, n1, n2 = parts[colour]
        if d > n2 // 2:
            return
        if 2 * d == n2 and way != (1 if j % 4 in (0, 3) else -1):
            return
        event = ("p2", colour, j, d)
        need[event] = 2 if 2 * d < n2 else 1
        outstanding.add(event)
        queue(("zy" if swap else "yz")[1] + "+-"[way < 0], n2 // 2 - d + extra[colour], colour, event,
              place(colour, ring_offsets(n1)[j], -way * (d - 1)))

    have = {c: set() for c in "abc"}

    def got(colour, g):
        have[colour].add(g)
        if colour == "c":
            event = ("x1", g)
            need[event] = 2
            outstanding.add(event)
            for way in "+-":
                queue("x" + way, 1, "c", event, g)

    def take(event):
        kind = event[0]
        if kind == "x1":
            g = event[1]
            way = "+-"[groups.index(g) % 2]
            queue("x" + way, 0, "c", ("x2", g), g)
            return
        colour = event[1]
        swap, n1, n2 = parts[colour]
        if kind == "p1":
            d = event[2]
            for way in ways(n1, d):
                put1(colour, d + 1, way)
                j = [o % n1 for o in ring_offsets(n1)].index(-way * d % n1)
                for w2 in (1, -1):
                    put2(colour, j, 1, w2)
                got(colour, place(colour, -way * d, 0))
        else:
            j, d = event[2:]
            for way in (1, -1) if 2 * d < n2 else ((1 if j % 4 in (0, 3) else -1),):
                put2(colour, j, d + 1, way)
                got(colour, place(colour, ring_offsets(n1)[j], -way * d))

    for colour in "cab":
        for way in (1, -1):
            put1(colour, 1, way)
        for way in (1, -1):
            put2(colour, 0, 1, way)
        got(colour, (0, 0))
    first_done, last_done = [], []
    while len(last_done) < len(groups):
        issue()
        ready = [e for e in outstanding if issued.get(e, 0) == need[e]]
        ready.sort(key=lambda e: (arrive[e], str(e)))
        if ready and arrive[ready[0]] <= now[0]:
            event = ready[0]
            outstanding.discard(event)
            ops.append(("take", event))
            now[0] += 0.03
            take(event)
            continue
        left = [g for g in groups if g not in first_done]
        one = [g for g in left if g in have["a"] and g in have["b"]][:most]
        todo = [g for g in groups if g not in last_done]
        two = [g for g in first_done if g not in last_done and issued.get(("x2", g)) and arrive[("x2", g)] <= now[0]][:most]
        if one and (len(one) >= least or len(one) == len(left)) and not (two and len(two) >= least):
            first_done.extend(one)
            ops.append(("first", tuple(one)))
            now[0] += 0.75 + 0.037 * len(one)
        elif two and (len(two) >= least or len(two) == len(todo)):
            last_done.extend(two)
            ops.append(("last", tuple(two)))
            now[0] += 0.9 + 0.045 * len(two)
        elif ready:
            now[0] = arrive[ready[0]]
        else:
            late = [arrive[("x2", g)] for g in todo if issued.get(("x2", g)) and arrive[("x2", g)] > now[0]]
            nxt = min(late) if late else None
            if nxt is None:
                nxt = min(free[l] for l in pending if pending[l]) - depth + 1e-6
            now[0] = max(nxt, now[0])
    return ops, need


def kernel(
    sizes, steps, need, hid_in, whbm, rhead_in, ids_in, lens_in, pids_in, out1, out2,
    hid, rhead, ids, lens, pids,
    wmat, abuf, bbuf, own, cbuf, quarter, acc, side, gath, gmeta, meta, tiles, got_z, got_y, got_x, sum_y, sum_x, pair, pgot,
    in_sem, w_send, w_recv, g_send, g_recv, m_send, m_recv, p_send, p_recv,
    a_send, b_send, c_send, o_send, e_recv, d_recv, z_send, z_recv, y_send, y_recv, x_send, x_recv,
):
    nx, ny, nz, ka, kb, kq = sizes
    rows = nx * 4
    voc = whbm.shape[1]
    y, z, x, c = (lax.axis_index(a) for a in (AXY, AXZ, AXX, AXC))

    def at(pos, off, n):
        return lax.rem(pos + (off % n), n)

    barrier = pltpu.get_barrier_semaphore()
    partners = [{AXX: at(x, d, nx)} for d in range(1, nx)]
    partners += [{AXY: at(y, d, ny)} for d in (1, -1)]
    partners += [{AXZ: at(z, d, nz)} for d in (1, -1)]
    partners += [{AXC: 1 - c}]
    for dev in partners:
        pl.semaphore_signal(barrier, inc=1, device_id=dev, device_id_type=MESH)

    loads = [
        pltpu.make_async_copy(src, dst, in_sem.at[i])
        for i, (src, dst) in enumerate((
            (hid_in, hid), (ids_in, ids), (lens_in, lens), (pids_in, pids), (rhead_in, rhead),
            (whbm, wmat.at[:, pl.ds(0, voc)]),
        ))
    ]
    for load in loads:
        load.start()
    loads[0].wait()
    loads[1].wait()

    row8 = lax.broadcasted_iota(jnp.int32, (8, LANES), 0)
    lane8 = lax.broadcasted_iota(jnp.int32, (8, LANES), 1)
    idv = jnp.zeros((8, LANES), jnp.int32)
    for t in range(4):
        idv = jnp.where(row8 == t, ids[t // 2, t % 2], idv)
    digits = jnp.where(lane8 == 0, idv >> 16, jnp.where(lane8 == 1, (idv >> 8) & 255, idv & 255))
    meta[...] = jnp.where(lane8 < 3, digits, 0).astype(F32)
    pl.semaphore_wait(barrier, len(partners))

    started = []

    def send(src, dst, ssem, rsem, dev, keep=True):
        copy = pltpu.make_async_remote_copy(
            src_ref=src, dst_ref=dst, send_sem=ssem, recv_sem=rsem, device_id=dev, device_id_type=MESH
        )
        copy.start()
        if keep:
            started.append(copy)

    def take(ref, sem):
        pltpu.make_async_copy(ref, ref, sem).wait()

    def take_tiles(n, sem):
        take(bbuf.at[pl.ds(0, n)], sem)

    for d in range(1, nx):
        send(hid, gath.at[x], g_send.at[d - 1], g_recv, {AXX: at(x, d, nx)})
    for d in range(1, nx):
        send(meta, gmeta.at[x], m_send, m_recv, {AXX: at(x, d, nx)}, keep=False)
    send(whbm, wmat.at[:, pl.ds(voc, voc)], w_send, w_recv, {AXC: 1 - c})

    gath[x] = hid[...]
    gmeta[x] = meta[...]

    for load in loads[2:5]:
        load.wait()
    rewards = []
    for r in range(2):
        both = sum(
            hid[r, :, pl.ds(k * LANES, LANES)].astype(F32) * rhead[k:k + 1].astype(F32)
            for k in range(rhead.shape[0])
        )
        both = jnp.sum(both, axis=1, keepdims=True)
        rewards.append(jnp.where(lens[r] == 1, both[0:1], both[1:2]))
    lane1 = lax.broadcasted_iota(jnp.int32, (1, LANES), 1)
    stacked = jnp.zeros((1, LANES), F32)
    for r in range(2):
        stacked += jnp.where(lane1 == pids[r], rewards[r], 0.0)
        stacked += jnp.where(lane1 == pids[r] + PROMPTS, rewards[r] * rewards[r], 0.0)
    pair[...] = jnp.where(row8 == 3, stacked, 0.0)

    take(gath.at[pl.ds(0, nx - 1)], g_recv)
    take(gmeta.at[pl.ds(0, nx - 1)], m_recv)

    whole = jnp.concatenate(
        [gath[i, r].astype(F32) for i in range(nx) for r in range(2)], axis=0
    ).astype(jnp.bfloat16)
    pieces = [whole[:, k * LANES:(k + 1) * LANES] for k in range(ka + kb + nx * kq)]
    for k in range(nx * kq):
        quarter[k // kq, k % kq] = pieces[ka + kb + k]
    base_a, base_b, base_o = (y * nz + z) * (ka + 1), (y * nz + z) * kb, (y * nz + z) * kq
    for k in range(ka):
        abuf[base_a + k] = pieces[k]
    for k in range(kb):
        bbuf[base_b + k] = pieces[ka + k]
    abuf[base_a + ka] = jnp.concatenate([gmeta[i, 0:4] for i in range(nx)], axis=0).astype(jnp.bfloat16)
    for k in range(kq):
        own[base_o + k] = quarter[x, k]

    send(pair, pgot, p_send, p_recv, {AXC: 1 - c})

    groups = [(dy % ny, dz % nz) for dy in ring_offsets(ny) for dz in ring_offsets(nz)]
    many = len(groups)
    where = {g: (at(y, g[0], ny), at(z, g[1], nz)) for g in groups}
    flat = {g: qy * nz + qz for g, (qy, qz) in where.items()}
    tiles_of = {"a": ka + 1, "b": kb, "c": kq}
    store = {"a": abuf, "b": bbuf, "c": own}
    out_sem = {"a": a_send, "b": b_send, "c": o_send}
    axis = {"x": (AXX, x, nx), "y": (AXY, y, ny), "z": (AXZ, z, nz)}
    index = {event: i for i, event in enumerate(sorted(need, key=str))}
    part_of = {g: n for n, op in enumerate([op for op in steps if op[0] == "last"]) for g in op[1]}

    def in_a(g, k=0):
        return flat[g] * (ka + 1) + k

    def in_b(g, k=0):
        return flat[g] * kb + k

    def in_c(r, g, k=0):
        return (r * many + flat[g]) * kq + k

    def block(colour, g):
        n = tiles_of[colour]
        return store[colour].at[pl.ds(flat[g] * n, n)]

    def put(link, event, g):
        name, pos, n = axis[link[0]]
        dev = {name: at(pos, 1 if link[1] == "+" else -1, n)}
        side_in = "+-".index(link[1])
        if event[0] == "x1":
            there = cbuf.at[pl.ds(in_c(side_in, g), kq)]
            send(block("c", g), there, c_send, e_recv.at[index[event]], dev, keep=False)
        elif event[0] == "x2":
            here, there = cbuf.at[pl.ds(in_c(side_in, g), kq)], cbuf.at[pl.ds(in_c(2, g), kq)]
            send(here, there, c_send, d_recv.at[part_of[g]], dev, keep=False)
        else:
            b = block(event[1], g)
            send(b, b, out_sem[event[1]], e_recv.at[index[event]], dev, keep=False)

    def get(event):
        take_tiles(need[event] * tiles_of["c" if event[0] == "x1" else event[1]], e_recv.at[index[event]])

    wide = 2 * LANES
    chip = ((y * nz + z) * nx + x) * 2
    turns = [at(x, off, nx) for off in (0, -1, 1, 2)]
    starts = [pl.multiple_of((ka + kb + q * kq) * LANES, LANES) for q in turns]

    def product(chunk, last):
        def step(n, carry):
            cols = pl.ds(pl.multiple_of(n * wide, wide), wide)
            left = []
            for i in chunk:
                if last:
                    parts = [own[flat[i] * kq + k] for k in range(kq)]
                    parts += [cbuf[in_c(r, i, k)] for r in range(3) for k in range(kq)]
                else:
                    parts = [abuf[in_a(i, k)] for k in range(ka)]
                    parts += [bbuf[in_b(i, k)] for k in range(kb)]
                left.append(jnp.concatenate(parts, axis=1))
            left = jnp.concatenate(left, axis=0)
            if last:
                right = jnp.concatenate([wmat[pl.ds(s, kq * LANES), cols] for s in starts], axis=0)
            else:
                right = wmat[pl.ds(0, (ka + kb) * LANES), cols]
            part = jnp.dot(left, right, preferred_element_type=F32)
            for m, i in enumerate(chunk):
                piece = part[m * rows:(m + 1) * rows]
                if last:
                    piece = acc[where[i] + (slice(None), cols)] + piece
                acc[where[i] + (slice(None), cols)] = piece
            return carry

        lax.fori_loop(0, 2 * voc // wide, step, 0)

    def score(chunk):
        toks = len(chunk) * rows

        def logits():
            return jnp.concatenate([acc[where[i]] for i in chunk], axis=0)

        lane = lax.broadcasted_iota(jnp.int32, (toks, 2 * voc), 1)
        entry = jnp.where(lane < voc, (chip + c) * voc + lane, (chip + 1 - c) * voc + lane - voc)
        lane_t = lax.broadcasted_iota(jnp.int32, (toks, LANES), 1)
        peak = jnp.max(logits(), axis=1, keepdims=True)
        total = jnp.sum(jnp.exp(logits() - peak), axis=1, keepdims=True)
        dig = jnp.concatenate([abuf[in_a(i, ka)] for i in chunk], axis=0).astype(F32)
        want = (dig[:, 0:1] * 65536.0 + dig[:, 1:2] * 256.0 + dig[:, 2:3]).astype(jnp.int32)
        picked = jnp.sum(jnp.where(entry == want, logits(), 0.0), axis=1, keepdims=True)
        out = jnp.where(lane_t == 0, peak, jnp.where(lane_t == 1, total, jnp.where(lane_t == 2, picked, 0.0)))
        for m, i in enumerate(chunk):
            side[where[i][1], where[i][0]] = out[m * rows:(m + 1) * rows]

    ready = False
    count = 0
    for op in steps:
        if op[0] == "send":
            put(*op[1:])
        elif op[0] == "take":
            get(op[1])
        elif op[0] == "first":
            if not ready:
                loads[5].wait()
                take(wmat.at[:, pl.ds(voc, voc)], w_recv)
                ready = True
            product(op[1], False)
            count += 1
        else:
            take_tiles(len(op[1]) * kq, d_recv.at[part_of[op[1][0]]])
            product(op[1], True)
            score(op[1])
            count += 1

    take(pgot, p_recv)
    prompt_row = pair[...] + pgot[...]

    def slab(q):
        block = side[q].reshape(ny * rows, LANES)
        if ny * rows < LANES:
            block = jnp.concatenate([block, jnp.zeros((LANES - ny * rows, LANES), F32)], axis=0)
        return jnp.where(row8 == 3, prompt_row, block.T[0:8, :])

    def step(i, carry):
        h = (i + 1) // 2
        d = nz // 2 + h * (1 - 2 * (i % 2))
        q = lax.rem(z + d, nz)
        tiles[i] = slab(q)
        pltpu.make_async_remote_copy(
            src_ref=tiles.at[i], dst_ref=got_z.at[i], send_sem=z_send, recv_sem=z_recv,
            device_id={AXZ: q}, device_id_type=MESH,
        ).start()
        return carry

    lax.fori_loop(0, nz - 1, step, 0)

    def merge(parts):
        top = functools.reduce(jnp.maximum, [p[0:1] for p in parts])
        out = sum(p * jnp.where(row8 == 1, jnp.exp(p[0:1] - top), 1.0) for p in parts)
        return jnp.where(row8 == 0, top, out)

    mine = slab(z)
    take(got_z, z_recv)
    sum_y[...] = merge([mine] + [got_z[i] for i in range(nz - 1)])
    far = sorted(range(1, ny), key=lambda d: -hops(ny, d))
    for d in far:
        send(sum_y, got_y.at[d - 1], y_send, y_recv, {AXY: at(y, d, ny)}, keep=False)
    take(got_y, y_recv)
    sum_x[...] = merge([sum_y[...]] + [got_y[d - 1] for d in range(1, ny)])
    far = sorted(range(1, nx), key=lambda d: -hops(nx, d))
    for d in far:
        send(sum_x, got_x.at[d - 1], x_send, x_recv, {AXX: at(x, d, nx)}, keep=False)
    take(got_x, x_recv)
    done = merge([sum_x[...]] + [got_x[d - 1] for d in range(1, nx)])

    logprob = done[2:3] - (done[0:1] + jnp.log(done[1:2]))
    base = y * rows + x * 4
    r_out = lax.broadcasted_iota(jnp.int32, (2, 2), 0)
    w_out = lax.broadcasted_iota(jnp.int32, (2, 2), 1)
    value = jnp.zeros((2, 2), F32)
    for t in range(4):
        r, w = t // 2, t % 2
        one = jnp.sum(jnp.where(lane1 == base + t, logprob, 0.0), axis=1, keepdims=True)
        one = jnp.where(w < lens[r], one, 0.0)
        value = jnp.where((r_out == r) & (w_out == w), one, value)
    out1[...] = value
    moment = done[3:4] * (1.0 / GROUP)
    spot = lax.broadcasted_iota(jnp.int32, (1, 2), 1)
    adv = jnp.zeros((1, 2), F32)
    for r in range(2):
        mean = jnp.sum(jnp.where(lane1 == pids[r], moment, 0.0), axis=1, keepdims=True)
        square = jnp.sum(jnp.where(lane1 == pids[r] + PROMPTS, moment, 0.0), axis=1, keepdims=True)
        scale = jnp.sqrt(jnp.maximum(square - mean * mean, 1.0))
        adv = jnp.where(spot == r, (rewards[r] - mean) / scale, adv)
    out2[...] = adv

    for copy in started:
        copy.wait_send()
    take_tiles((many - 1) * (ka + 1), a_send)
    take_tiles((many - 1) * kq, o_send)
    take_tiles((many - 1) * kb, b_send)
    take(cbuf, c_send)
    for n, sem in ((nz - 1, z_send), (ny - 1, y_send), (nx - 1, x_send), (nx - 1, m_send)):
        take_tiles(n, sem)


def local(hidden, lm_head, reward_head, target_ids, lengths, prompt_ids):
    nx, ny, nz = (lax.axis_size(a) for a in (AXX, AXY, AXZ))
    width, voc = lm_head.shape
    tiles = width // LANES
    kq = max(1, tiles * 3 // (7 * nx))
    ka = (tiles - kq * nx) * 3 // 8
    kb = tiles - kq * nx - ka
    rows = nx * 4
    size = rows * LANES * 2
    steps, need = plan(ny, nz, {"a": (ka + 1) * size, "b": kb * size, "c": kq * size})
    lasts = sum(op[0] == "last" for op in steps)
    dma = pltpu.SemaphoreType.DMA
    vmem = pl.BlockSpec(memory_space=pltpu.VMEM)
    tile = (8, LANES)
    out1, out2 = pl.pallas_call(
        functools.partial(kernel, (nx, ny, nz, ka, kb, kq), steps, need),
        out_shape=(jax.ShapeDtypeStruct((2, 2), F32), jax.ShapeDtypeStruct((1, 2), F32)),
        in_specs=[pl.BlockSpec(memory_space=pl.ANY)] * 6,
        out_specs=(vmem, vmem),
        scratch_shapes=[
            pltpu.VMEM((2, 2, width), jnp.bfloat16),
            pltpu.VMEM((tiles, LANES), jnp.bfloat16),
            pltpu.SMEM((2, 2), jnp.int32),
            pltpu.SMEM((2,), jnp.int32),
            pltpu.SMEM((2,), jnp.int32),
            pltpu.VMEM((width, 2 * voc), jnp.bfloat16),
            pltpu.VMEM((ny * nz * (ka + 1), rows, LANES), jnp.bfloat16),
            pltpu.VMEM((ny * nz * kb, rows, LANES), jnp.bfloat16),
            pltpu.VMEM((ny * nz * kq, rows, LANES), jnp.bfloat16),
            pltpu.VMEM((3 * ny * nz * kq, rows, LANES), jnp.bfloat16),
            pltpu.VMEM((nx, kq, rows, LANES), jnp.bfloat16),
            pltpu.VMEM((ny, nz, rows, 2 * voc), F32),
            pltpu.VMEM((nz, ny, rows, LANES), F32),
            pltpu.VMEM((nx, 2, 2, width), jnp.bfloat16),
            pltpu.VMEM((nx,) + tile, F32),
            pltpu.VMEM(tile, F32),
            pltpu.VMEM((nz - 1,) + tile, F32),
            pltpu.VMEM((nz - 1,) + tile, F32),
            pltpu.VMEM((ny - 1,) + tile, F32),
            pltpu.VMEM((nx - 1,) + tile, F32),
            pltpu.VMEM(tile, F32),
            pltpu.VMEM(tile, F32),
            pltpu.VMEM(tile, F32),
            pltpu.VMEM(tile, F32),
            dma((6,)), dma, dma,
            dma((nx - 1,)), dma, dma, dma,
            dma, dma,
            dma, dma, dma, dma, dma((len(need),)), dma((lasts,)),
            dma, dma, dma, dma, dma, dma,
        ],
        compiler_params=pltpu.CompilerParams(collective_id=0, has_side_effects=True),
        name="gather_score",
    )(hidden, lm_head, reward_head.reshape(tiles, LANES), target_ids, lengths, prompt_ids)
    return out1, out2.reshape(2)


def solution(mesh):
    split = Mesh(mesh.devices.reshape(mesh.shape["rep"], 8, 4, 2), REP_DP)
    placed = (P(REP_DP, None, None), P(None, REP_DP), P(), P(REP_DP, None), P(REP_DP), P(REP_DP))
    return jax.shard_map(
        local, mesh=split, in_specs=placed, out_specs=(P(REP_DP, None), P(REP_DP)), check_vma=False
    )
```

```python
import functools

import jax
import jax.numpy as jnp
from jax import lax
from jax.experimental import pallas as pl
from jax.experimental.pallas import tpu as pltpu
from jax.sharding import Mesh
from jax.sharding import PartitionSpec as P

GROUP = 16
PROMPTS = 64
REP_DP = ("rep", "dp_0", "dp_1", "dp_2")
AXY, AXZ, AXX, AXC = REP_DP
LANES = 128
MESH = pl.DeviceIdType.MESH
F32 = jnp.float32


def ring_offsets(n):
    order = [0]
    for d in range(1, n // 2 + 1):
        order.append(-d)
        if 2 * d < n:
            order.append(d)
    return order


def hops(n, off):
    return min(off % n, -off % n)


def plan(ny, nz, sizes, depth=1.5, rate=46.6e3, lag=2.2, least=8, most=16):
    parts = {"a": (0, ny, nz), "b": (1, nz, ny), "c": (0, ny, nz)}
    groups = [(dy % ny, dz % nz) for dy in ring_offsets(ny) for dz in ring_offsets(nz)]
    now, free, pending, issued, arrive = [0.0], {}, {}, {}, {}
    ops = []
    extra = {"a": 0, "b": 0, "c": 2}

    def queue(link, left, colour, event, what):
        pending.setdefault(link, []).append((-left, len(ops), colour, event, what))

    def issue():
        for link, wait in sorted(pending.items()):
            while wait and free.get(link, 0.0) - now[0] < depth:
                wait.sort(key=lambda w: w[0])
                left, _, colour, event, what = wait.pop(0)
                start = max(now[0], free.get(link, 0.0))
                free[link] = start + sizes[colour] / rate
                arrive[event] = max(arrive.get(event, 0.0), free[link] + lag)
                issued[event] = issued.get(event, 0) + 1
                ops.append(("send", link, event, what))

    def place(colour, off1, off2):
        swap, n1, n2 = parts[colour]
        return (off2 % n2, off1 % n1) if swap else (off1 % n1, off2 % n2)

    def ways(n, d):
        return (1, -1) if 2 * d < n else (1,)

    need, outstanding = {}, set()

    def put1(colour, d, way):
        swap, n1, n2 = parts[colour]
        if d <= n1 // 2 and way in ways(n1, d):
            event = ("p1", colour, d)
            need[event] = len(ways(n1, d))
            outstanding.add(event)
            queue(("zy" if swap else "yz")[0] + "+-"[way < 0], n1 // 2 - d + n2 // 2 + extra[colour], colour, event,
                  place(colour, -way * (d - 1), 0))

    def put2(colour, j, d, way):
        swap, n1, n2 = parts[colour]
        if d > n2 // 2:
            return
        if 2 * d == n2 and way != (1 if j % 4 in (0, 3) else -1):
            return
        event = ("p2", colour, j, d)
        need[event] = 2 if 2 * d < n2 else 1
        outstanding.add(event)
        queue(("zy" if swap else "yz")[1] + "+-"[way < 0], n2 // 2 - d + extra[colour], colour, event,
              place(colour, ring_offsets(n1)[j], -way * (d - 1)))

    have = {c: set() for c in "abc"}

    def got(colour, g):
        have[colour].add(g)
        if colour == "c":
            event = ("x1", g)
            need[event] = 2
            outstanding.add(event)
            for way in "+-":
                queue("x" + way, 1, "c", event, g)

    def take(event):
        kind = event[0]
        if kind == "x1":
            g = event[1]
            way = "+-"[groups.index(g) % 2]
            queue("x" + way, 0, "c", ("x2", g), g)
            return
        colour = event[1]
        swap, n1, n2 = parts[colour]
        if kind == "p1":
            d = event[2]
            for way in ways(n1, d):
                put1(colour, d + 1, way)
                j = [o % n1 for o in ring_offsets(n1)].index(-way * d % n1)
                for w2 in (1, -1):
                    put2(colour, j, 1, w2)
                got(colour, place(colour, -way * d, 0))
        else:
            j, d = event[2:]
            for way in (1, -1) if 2 * d < n2 else ((1 if j % 4 in (0, 3) else -1),):
                put2(colour, j, d + 1, way)
                got(colour, place(colour, ring_offsets(n1)[j], -way * d))

    for colour in "cab":
        for way in (1, -1):
            put1(colour, 1, way)
        for way in (1, -1):
            put2(colour, 0, 1, way)
        got(colour, (0, 0))
    first_done, last_done = [], []
    while len(last_done) < len(groups):
        issue()
        ready = [e for e in outstanding if issued.get(e, 0) == need[e]]
        ready.sort(key=lambda e: (arrive[e], str(e)))
        if ready and arrive[ready[0]] <= now[0]:
            event = ready[0]
            outstanding.discard(event)
            ops.append(("take", event))
            now[0] += 0.03
            take(event)
            continue
        left = [g for g in groups if g not in first_done]
        one = [g for g in left if g in have["a"] and g in have["b"]][:most]
        todo = [g for g in groups if g not in last_done]
        two = [g for g in first_done if g not in last_done and issued.get(("x2", g)) and arrive[("x2", g)] <= now[0]][:most]
        if one and (len(one) >= least or len(one) == len(left)) and not (two and len(two) >= least):
            first_done.extend(one)
            ops.append(("first", tuple(one)))
            now[0] += 0.75 + 0.037 * len(one)
        elif two and (len(two) >= least or len(two) == len(todo)):
            last_done.extend(two)
            ops.append(("last", tuple(two)))
            now[0] += 0.9 + 0.045 * len(two)
        elif ready:
            now[0] = arrive[ready[0]]
        else:
            late = [arrive[("x2", g)] for g in todo if issued.get(("x2", g)) and arrive[("x2", g)] > now[0]]
            nxt = min(late) if late else None
            if nxt is None:
                nxt = min(free[l] for l in pending if pending[l]) - depth + 1e-6
            now[0] = max(nxt, now[0])
    return ops, need


def kernel(
    sizes, steps, need, hid_in, whbm, rhead_in, ids_in, lens_in, pids_in, out1, out2,
    hid, rhead, ids, lens, pids,
    wmat, abuf, bbuf, own, cbuf, quarter, acc, side, gath, gmeta, meta, tiles, got_z, got_yx, sums, pair, pgot,
    in_sem, w_send, w_recv, g_send, g_recv, m_send, m_recv, p_send, p_recv,
    a_send, b_send, c_send, o_send, e_recv, d_recv, z_send, z_recv, y_send, y_recv,
):
    nx, ny, nz, ka, kb, kq = sizes
    rows = nx * 4
    voc = whbm.shape[1]
    y, z, x, c = (lax.axis_index(a) for a in (AXY, AXZ, AXX, AXC))

    def at(pos, off, n):
        return lax.rem(pos + (off % n), n)

    barrier = pltpu.get_barrier_semaphore()
    partners = [{AXX: at(x, d, nx)} for d in range(1, nx)]
    partners += [{AXY: at(y, d, ny)} for d in (1, -1)]
    partners += [{AXZ: at(z, d, nz)} for d in (1, -1)]
    partners += [{AXC: 1 - c}]
    for dev in partners:
        pl.semaphore_signal(barrier, inc=1, device_id=dev, device_id_type=MESH)

    loads = [
        pltpu.make_async_copy(src, dst, in_sem.at[i])
        for i, (src, dst) in enumerate((
            (hid_in, hid), (ids_in, ids), (lens_in, lens), (pids_in, pids), (rhead_in, rhead),
            (whbm, wmat.at[:, pl.ds(0, voc)]),
        ))
    ]
    for load in loads:
        load.start()
    loads[0].wait()
    loads[1].wait()

    row8 = lax.broadcasted_iota(jnp.int32, (8, LANES), 0)
    lane8 = lax.broadcasted_iota(jnp.int32, (8, LANES), 1)
    idv = jnp.zeros((8, LANES), jnp.int32)
    for t in range(4):
        idv = jnp.where(row8 == t, ids[t // 2, t % 2], idv)
    digits = jnp.where(lane8 == 0, idv >> 16, jnp.where(lane8 == 1, (idv >> 8) & 255, idv & 255))
    meta[...] = jnp.where(lane8 < 3, digits, 0).astype(F32)
    pl.semaphore_wait(barrier, len(partners))

    started = []

    def send(src, dst, ssem, rsem, dev, keep=True):
        copy = pltpu.make_async_remote_copy(
            src_ref=src, dst_ref=dst, send_sem=ssem, recv_sem=rsem, device_id=dev, device_id_type=MESH
        )
        copy.start()
        if keep:
            started.append(copy)

    def take(ref, sem):
        pltpu.make_async_copy(ref, ref, sem).wait()

    def take_tiles(n, sem):
        take(bbuf.at[pl.ds(0, n)], sem)

    for d in range(1, nx):
        send(hid, gath.at[x], g_send.at[d - 1], g_recv, {AXX: at(x, d, nx)})
    for d in range(1, nx):
        send(meta, gmeta.at[x], m_send, m_recv, {AXX: at(x, d, nx)}, keep=False)
    send(whbm, wmat.at[:, pl.ds(voc, voc)], w_send, w_recv, {AXC: 1 - c})

    gath[x] = hid[...]
    gmeta[x] = meta[...]

    for load in loads[2:5]:
        load.wait()
    rewards = []
    for r in range(2):
        both = sum(
            hid[r, :, pl.ds(k * LANES, LANES)].astype(F32) * rhead[k:k + 1].astype(F32)
            for k in range(rhead.shape[0])
        )
        both = jnp.sum(both, axis=1, keepdims=True)
        rewards.append(jnp.where(lens[r] == 1, both[0:1], both[1:2]))
    lane1 = lax.broadcasted_iota(jnp.int32, (1, LANES), 1)
    stacked = jnp.zeros((1, LANES), F32)
    for r in range(2):
        stacked += jnp.where(lane1 == pids[r], rewards[r], 0.0)
        stacked += jnp.where(lane1 == pids[r] + PROMPTS, rewards[r] * rewards[r], 0.0)
    pair[...] = jnp.where(row8 == 3, stacked, 0.0)

    take(gath.at[pl.ds(0, nx - 1)], g_recv)
    take(gmeta.at[pl.ds(0, nx - 1)], m_recv)

    whole = jnp.concatenate(
        [gath[i, r].astype(F32) for i in range(nx) for r in range(2)], axis=0
    ).astype(jnp.bfloat16)
    pieces = [whole[:, k * LANES:(k + 1) * LANES] for k in range(ka + kb + nx * kq)]
    for k in range(nx * kq):
        quarter[k // kq, k % kq] = pieces[ka + kb + k]
    base_a, base_b, base_o = (y * nz + z) * (ka + 1), (y * nz + z) * kb, (y * nz + z) * kq
    for k in range(ka):
        abuf[base_a + k] = pieces[k]
    for k in range(kb):
        bbuf[base_b + k] = pieces[ka + k]
    abuf[base_a + ka] = jnp.concatenate([gmeta[i, 0:4] for i in range(nx)], axis=0).astype(jnp.bfloat16)
    for k in range(kq):
        own[base_o + k] = quarter[x, k]

    send(pair, pgot, p_send, p_recv, {AXC: 1 - c})

    groups = [(dy % ny, dz % nz) for dy in ring_offsets(ny) for dz in ring_offsets(nz)]
    many = len(groups)
    where = {g: (at(y, g[0], ny), at(z, g[1], nz)) for g in groups}
    flat = {g: qy * nz + qz for g, (qy, qz) in where.items()}
    tiles_of = {"a": ka + 1, "b": kb, "c": kq}
    store = {"a": abuf, "b": bbuf, "c": own}
    out_sem = {"a": a_send, "b": b_send, "c": o_send}
    axis = {"x": (AXX, x, nx), "y": (AXY, y, ny), "z": (AXZ, z, nz)}
    index = {event: i for i, event in enumerate(sorted(need, key=str))}
    part_of = {g: n for n, op in enumerate([op for op in steps if op[0] == "last"]) for g in op[1]}

    def in_a(g, k=0):
        return flat[g] * (ka + 1) + k

    def in_b(g, k=0):
        return flat[g] * kb + k

    def in_c(r, g, k=0):
        return (r * many + flat[g]) * kq + k

    def block(colour, g):
        n = tiles_of[colour]
        return store[colour].at[pl.ds(flat[g] * n, n)]

    def put(link, event, g):
        name, pos, n = axis[link[0]]
        dev = {name: at(pos, 1 if link[1] == "+" else -1, n)}
        side_in = "+-".index(link[1])
        if event[0] == "x1":
            there = cbuf.at[pl.ds(in_c(side_in, g), kq)]
            send(block("c", g), there, c_send, e_recv.at[index[event]], dev, keep=False)
        elif event[0] == "x2":
            here, there = cbuf.at[pl.ds(in_c(side_in, g), kq)], cbuf.at[pl.ds(in_c(2, g), kq)]
            send(here, there, c_send, d_recv.at[part_of[g]], dev, keep=False)
        else:
            b = block(event[1], g)
            send(b, b, out_sem[event[1]], e_recv.at[index[event]], dev, keep=False)

    def get(event):
        take_tiles(need[event] * tiles_of["c" if event[0] == "x1" else event[1]], e_recv.at[index[event]])

    wide = 2 * LANES
    chip = ((y * nz + z) * nx + x) * 2
    turns = [at(x, off, nx) for off in (0, -1, 1, 2)]
    starts = [pl.multiple_of((ka + kb + q * kq) * LANES, LANES) for q in turns]

    def product(chunk, last):
        def step(n, carry):
            cols = pl.ds(n * wide, wide)
            left = []
            for i in chunk:
                if last:
                    parts = [own[flat[i] * kq + k] for k in range(kq)]
                    parts += [cbuf[in_c(r, i, k)] for r in range(3) for k in range(kq)]
                else:
                    parts = [abuf[in_a(i, k)] for k in range(ka)]
                    parts += [bbuf[in_b(i, k)] for k in range(kb)]
                left.append(jnp.concatenate(parts, axis=1))
            left = jnp.concatenate(left, axis=0)
            if last:
                right = jnp.concatenate([wmat[pl.ds(s, kq * LANES), cols] for s in starts], axis=0)
            else:
                right = wmat[pl.ds(0, (ka + kb) * LANES), cols]
            part = jnp.dot(left, right, preferred_element_type=F32)
            for m, i in enumerate(chunk):
                piece = part[m * rows:(m + 1) * rows]
                if last:
                    piece = acc[where[i] + (slice(None), cols)] + piece
                acc[where[i] + (slice(None), cols)] = piece
            return carry

        for n in range(2 * voc // wide):
            step(n, 0)

    def score(chunk):
        toks = len(chunk) * rows

        def logits():
            return jnp.concatenate([acc[where[i]] for i in chunk], axis=0)

        lane = lax.broadcasted_iota(jnp.int32, (toks, 2 * voc), 1)
        entry = jnp.where(lane < voc, (chip + c) * voc + lane, (chip + 1 - c) * voc + lane - voc)
        lane_t = lax.broadcasted_iota(jnp.int32, (toks, LANES), 1)
        peak = jnp.max(logits(), axis=1, keepdims=True)
        total = jnp.sum(jnp.exp(logits() - peak), axis=1, keepdims=True)
        dig = jnp.concatenate([abuf[in_a(i, ka)] for i in chunk], axis=0).astype(F32)
        want = (dig[:, 0:1] * 65536.0 + dig[:, 1:2] * 256.0 + dig[:, 2:3]).astype(jnp.int32)
        picked = jnp.sum(jnp.where(entry == want, logits(), 0.0), axis=1, keepdims=True)
        out = jnp.where(lane_t == 0, peak, jnp.where(lane_t == 1, total, jnp.where(lane_t == 2, picked, 0.0)))
        for m, i in enumerate(chunk):
            side[where[i][1], where[i][0]] = out[m * rows:(m + 1) * rows]

    ready = False
    count = 0
    for op in steps:
        if op[0] == "send":
            put(*op[1:])
        elif op[0] == "take":
            get(op[1])
        elif op[0] == "first":
            if not ready:
                loads[5].wait()
                take(wmat.at[:, pl.ds(voc, voc)], w_recv)
                ready = True
            product(op[1], False)
            count += 1
        else:
            take_tiles(len(op[1]) * kq, d_recv.at[part_of[op[1][0]]])
            product(op[1], True)
            score(op[1])
            count += 1

    take(pgot, p_recv)
    prompt_row = pair[...] + pgot[...]

    def slab(q):
        block = side[q].reshape(ny * rows, LANES)
        if ny * rows < LANES:
            block = jnp.concatenate([block, jnp.zeros((LANES - ny * rows, LANES), F32)], axis=0)
        return jnp.where(row8 == 3, prompt_row, block.T[0:8, :])

    def step(i, carry):
        h = (i + 1) // 2
        d = nz // 2 + h * (1 - 2 * (i % 2))
        q = lax.rem(z + d, nz)
        tiles[i] = slab(q)
        pltpu.make_async_remote_copy(
            src_ref=tiles.at[i], dst_ref=got_z.at[i], send_sem=z_send, recv_sem=z_recv,
            device_id={AXZ: q}, device_id_type=MESH,
        ).start()
        return carry

    lax.fori_loop(0, nz - 1, step, 0)

    def merge(parts):
        row8 = lax.broadcasted_iota(jnp.int32, parts[0].shape, 0)
        top = functools.reduce(jnp.maximum, [p[0:1] for p in parts])
        out = sum(p * jnp.where(row8 == 1, jnp.exp(p[0:1] - top), 1.0) for p in parts)
        return jnp.where(row8 == 0, top, out)

    mine = slab(z)
    take(got_z, z_recv)
    sums[...] = merge([mine] + [got_z[i] for i in range(nz - 1)])[0:4]
    others = [(dy, dx) for dy in range(ny) for dx in range(nx) if dy or dx]
    for n, (dy, dx) in sorted(enumerate(others), key=lambda o: -hops(ny, o[1][0]) - hops(nx, o[1][1])):
        send(sums, got_yx.at[n], y_send, y_recv, {AXY: at(y, dy, ny), AXX: at(x, dx, nx)}, keep=False)
    take(got_yx, y_recv)
    done = merge([sums[...]] + [got_yx[n] for n in range(len(others))])

    logprob = done[2:3] - (done[0:1] + jnp.log(done[1:2]))
    base = y * rows + x * 4
    r_out = lax.broadcasted_iota(jnp.int32, (2, 2), 0)
    w_out = lax.broadcasted_iota(jnp.int32, (2, 2), 1)
    value = jnp.zeros((2, 2), F32)
    for t in range(4):
        r, w = t // 2, t % 2
        one = jnp.sum(jnp.where(lane1 == base + t, logprob, 0.0), axis=1, keepdims=True)
        one = jnp.where(w < lens[r], one, 0.0)
        value = jnp.where((r_out == r) & (w_out == w), one, value)
    out1[...] = value
    moment = done[3:4] * (1.0 / GROUP)
    spot = lax.broadcasted_iota(jnp.int32, (1, 2), 1)
    adv = jnp.zeros((1, 2), F32)
    for r in range(2):
        mean = jnp.sum(jnp.where(lane1 == pids[r], moment, 0.0), axis=1, keepdims=True)
        square = jnp.sum(jnp.where(lane1 == pids[r] + PROMPTS, moment, 0.0), axis=1, keepdims=True)
        scale = jnp.sqrt(jnp.maximum(square - mean * mean, 1.0))
        adv = jnp.where(spot == r, (rewards[r] - mean) / scale, adv)
    out2[...] = adv

    for copy in started:
        copy.wait_send()
    take_tiles((many - 1) * (ka + 1), a_send)
    take_tiles((many - 1) * kq, o_send)
    take_tiles((many - 1) * kb, b_send)
    take(cbuf, c_send)
    take_tiles(nz - 1, z_send)
    take_tiles(nx - 1, m_send)
    take(got_yx, y_send)


def local(hidden, lm_head, reward_head, target_ids, lengths, prompt_ids):
    nx, ny, nz = (lax.axis_size(a) for a in (AXX, AXY, AXZ))
    width, voc = lm_head.shape
    tiles = width // LANES
    kq = max(1, tiles * 3 // (7 * nx))
    ka = (tiles - kq * nx) * 3 // 8
    kb = tiles - kq * nx - ka
    rows = nx * 4
    size = rows * LANES * 2
    steps, need = plan(ny, nz, {"a": (ka + 1) * size, "b": kb * size, "c": kq * size})
    lasts = sum(op[0] == "last" for op in steps)
    dma = pltpu.SemaphoreType.DMA
    vmem = pl.BlockSpec(memory_space=pltpu.VMEM)
    tile = (8, LANES)
    out1, out2 = pl.pallas_call(
        functools.partial(kernel, (nx, ny, nz, ka, kb, kq), steps, need),
        out_shape=(pltpu.VMEM((2, 2), F32), pltpu.VMEM((1, 2), F32)),
        in_specs=[pl.BlockSpec(memory_space=pl.ANY)] * 6,
        out_specs=(vmem, vmem),
        scratch_shapes=[
            pltpu.VMEM((2, 2, width), jnp.bfloat16),
            pltpu.VMEM((tiles, LANES), jnp.bfloat16),
            pltpu.SMEM((2, 2), jnp.int32),
            pltpu.SMEM((2,), jnp.int32),
            pltpu.SMEM((2,), jnp.int32),
            pltpu.VMEM((width, 2 * voc), jnp.bfloat16),
            pltpu.VMEM((ny * nz * (ka + 1), rows, LANES), jnp.bfloat16),
            pltpu.VMEM((ny * nz * kb, rows, LANES), jnp.bfloat16),
            pltpu.VMEM((ny * nz * kq, rows, LANES), jnp.bfloat16),
            pltpu.VMEM((3 * ny * nz * kq, rows, LANES), jnp.bfloat16),
            pltpu.VMEM((nx, kq, rows, LANES), jnp.bfloat16),
            pltpu.VMEM((ny, nz, rows, 2 * voc), F32),
            pltpu.VMEM((nz, ny, rows, LANES), F32),
            pltpu.VMEM((nx, 2, 2, width), jnp.bfloat16),
            pltpu.VMEM((nx,) + tile, F32),
            pltpu.VMEM(tile, F32),
            pltpu.VMEM((nz - 1,) + tile, F32),
            pltpu.VMEM((nz - 1,) + tile, F32),
            pltpu.VMEM((ny * nx - 1, 4, LANES), F32),
            pltpu.VMEM((4, LANES), F32),
            pltpu.VMEM(tile, F32),
            pltpu.VMEM(tile, F32),
            dma((6,)), dma, dma,
            dma((nx - 1,)), dma, dma, dma,
            dma, dma,
            dma, dma, dma, dma, dma((len(need),)), dma((lasts,)),
            dma, dma, dma, dma,
        ],
        compiler_params=pltpu.CompilerParams(collective_id=0, has_side_effects=True),
        name="gather_score",
    )(hidden, lm_head, reward_head.reshape(tiles, LANES), target_ids, lengths, prompt_ids)
    return out1, out2.reshape(2)


def solution(mesh):
    split = Mesh(mesh.devices.reshape(mesh.shape["rep"], 8, 4, 2), REP_DP)
    placed = (P(REP_DP, None, None), P(None, REP_DP), P(), P(REP_DP, None), P(REP_DP), P(REP_DP))
    return jax.shard_map(
        local, mesh=split, in_specs=placed, out_specs=(P(REP_DP, None), P(REP_DP)), check_vma=False
    )
```

```python
import functools

import jax
import jax.numpy as jnp
from jax import lax
from jax.experimental import pallas as pl
from jax.experimental.pallas import tpu as pltpu
from jax.sharding import Mesh
from jax.sharding import PartitionSpec as P

GROUP = 16
PROMPTS = 64
REP_DP = ("rep", "dp_0", "dp_1", "dp_2")
AXY, AXZ, AXX, AXC = REP_DP
LANES = 128
MESH = pl.DeviceIdType.MESH
F32 = jnp.float32


def ring_offsets(n):
    order = [0]
    for d in range(1, n // 2 + 1):
        order.append(-d)
        if 2 * d < n:
            order.append(d)
    return order


def hops(n, off):
    return min(off % n, -off % n)


def plan(ny, nz, sizes, depth=0.8, rate=46.6e3, lag=2.4, least=(12, 8), most=16, tail=24):
    parts = {"a": (0, ny, nz), "b": (1, nz, ny), "c": (0, ny, nz)}
    groups = [(dy % ny, dz % nz) for dy in ring_offsets(ny) for dz in ring_offsets(nz)]
    now, free, pending, issued, arrive = [0.0], {}, {}, {}, {}
    ops = []
    extra = {"a": 0, "b": 0, "c": 2}

    def queue(link, left, colour, event, what):
        pending.setdefault(link, []).append((-left, len(ops), colour, event, what))

    def issue():
        for link, wait in sorted(pending.items()):
            while wait and free.get(link, 0.0) - now[0] < depth:
                wait.sort(key=lambda w: w[0])
                left, _, colour, event, what = wait.pop(0)
                start = max(now[0], free.get(link, 0.0))
                free[link] = start + sizes[colour] / rate
                arrive[event] = max(arrive.get(event, 0.0), free[link] + lag)
                issued[event] = issued.get(event, 0) + 1
                ops.append(("send", link, event, what))
                now[0] += 0.015

    def place(colour, off1, off2):
        swap, n1, n2 = parts[colour]
        return (off2 % n2, off1 % n1) if swap else (off1 % n1, off2 % n2)

    def ways(n, d):
        return (1, -1) if 2 * d < n else (1,)

    need, outstanding = {}, set()

    def put1(colour, d, way):
        swap, n1, n2 = parts[colour]
        if d <= n1 // 2 and way in ways(n1, d):
            event = ("p1", colour, d)
            need[event] = len(ways(n1, d))
            outstanding.add(event)
            queue(("zy" if swap else "yz")[0] + "+-"[way < 0], n1 // 2 - d + n2 // 2 + extra[colour], colour, event,
                  place(colour, -way * (d - 1), 0))

    def put2(colour, j, d, way):
        swap, n1, n2 = parts[colour]
        if d > n2 // 2:
            return
        if 2 * d == n2 and way != (1 if j % 4 in (0, 3) else -1):
            return
        event = ("p2", colour, j, d)
        need[event] = 2 if 2 * d < n2 else 1
        outstanding.add(event)
        queue(("zy" if swap else "yz")[1] + "+-"[way < 0], n2 // 2 - d + extra[colour], colour, event,
              place(colour, ring_offsets(n1)[j], -way * (d - 1)))

    have = {c: set() for c in "abc"}
    batch, done = {}, []

    def got(colour, new):
        have[colour].update(new)
        if colour == "c":
            event = ("x1",) + new[0]
            need[event] = 2 * len(new)
            batch[event] = new
            outstanding.add(event)
            for g in new:
                for way in "+-":
                    queue("x" + way, 1, "c", event, g)

    def take(event):
        kind = event[0]
        if kind == "x1":
            for n, g in enumerate(batch[event]):
                queue("x" + "+-"[(n + len(done)) % 2], 0, "c", ("x2", g), g)
            done.append(event)
            return
        colour = event[1]
        swap, n1, n2 = parts[colour]
        if kind == "p1":
            d = event[2]
            for way in ways(n1, d):
                put1(colour, d + 1, way)
                j = [o % n1 for o in ring_offsets(n1)].index(-way * d % n1)
                for w2 in (1, -1):
                    put2(colour, j, 1, w2)
            got(colour, [place(colour, -way * d, 0) for way in ways(n1, d)])
        else:
            j, d = event[2:]
            sides = (1, -1) if 2 * d < n2 else ((1 if j % 4 in (0, 3) else -1),)
            for way in sides:
                put2(colour, j, d + 1, way)
            got(colour, [place(colour, ring_offsets(n1)[j], -way * d) for way in sides])

    for colour in "cab":
        for way in (1, -1):
            put1(colour, 1, way)
        for way in (1, -1):
            put2(colour, 0, 1, way)
        got(colour, [(0, 0)])
    first_done, last_done = [], []
    while len(last_done) < len(groups):
        issue()
        ready = [e for e in outstanding if issued.get(e, 0) == need[e]]
        ready.sort(key=lambda e: (arrive[e], str(e)))
        if ready and arrive[ready[0]] <= now[0]:
            event = ready[0]
            outstanding.discard(event)
            ops.append(("take", event))
            now[0] += 0.03
            take(event)
            continue
        left = [g for g in groups if g not in first_done]
        one = [g for g in left if g in have["a"] and g in have["b"]][:most]
        todo = [g for g in groups if g not in last_done]
        two = [g for g in first_done if g not in last_done and issued.get(("x2", g)) and arrive[("x2", g)] <= now[0]][:most]
        if one and (len(one) >= least[len(left) <= tail] or len(one) == len(left)) and not (two and len(two) >= least[len(todo) <= tail]):
            first_done.extend(one)
            ops.append(("first", tuple(one)))
            now[0] += 0.57 + 0.02 * len(one)
        elif two and (len(two) >= least[len(todo) <= tail] or len(two) == len(todo)):
            last_done.extend(two)
            ops.append(("last", tuple(two)))
            now[0] += 0.6 + 0.028 * len(two)
        elif ready:
            now[0] = arrive[ready[0]]
        else:
            late = [arrive[("x2", g)] for g in todo if issued.get(("x2", g)) and arrive[("x2", g)] > now[0]]
            nxt = min(late) if late else None
            if nxt is None:
                nxt = min(free[l] for l in pending if pending[l]) - depth + 1e-6
            now[0] = max(nxt, now[0])
    return ops, need


def kernel(
    sizes, steps, need, hid_in, whbm, rhead_in, ids_in, lens_in, pids_in, out1, out2,
    hid, rhead, ids, lens, pids,
    wmat, abuf, bbuf, own, cbuf, quarter, acc, side, gath, gmeta, meta, tiles, got_z, got_yx, sums, pair, pgot,
    in_sem, w_send, w_recv, g_send, g_recv, m_send, m_recv, p_send, p_recv,
    a_send, b_send, c_send, o_send, e_recv, d_recv, z_send, z_recv, y_send, y_recv,
):
    nx, ny, nz, ka, kb, kq = sizes
    rows = nx * 4
    voc = whbm.shape[1]
    y, z, x, c = (lax.axis_index(a) for a in (AXY, AXZ, AXX, AXC))

    def at(pos, off, n):
        return lax.rem(pos + (off % n), n)

    barrier = pltpu.get_barrier_semaphore()
    partners = [{AXX: at(x, d, nx)} for d in range(1, nx)]
    partners += [{AXY: at(y, d, ny)} for d in (1, -1)]
    partners += [{AXZ: at(z, d, nz)} for d in (1, -1)]
    partners += [{AXC: 1 - c}]
    for dev in partners:
        pl.semaphore_signal(barrier, inc=1, device_id=dev, device_id_type=MESH)

    loads = [
        pltpu.make_async_copy(src, dst, in_sem.at[i])
        for i, (src, dst) in enumerate((
            (hid_in, hid), (ids_in, ids), (lens_in, lens), (pids_in, pids), (rhead_in, rhead),
            (whbm, wmat.at[:, pl.ds(0, voc)]),
        ))
    ]
    for load in loads:
        load.start()
    loads[0].wait()
    loads[1].wait()

    row8 = lax.broadcasted_iota(jnp.int32, (8, LANES), 0)
    lane8 = lax.broadcasted_iota(jnp.int32, (8, LANES), 1)
    idv = jnp.zeros((8, LANES), jnp.int32)
    for t in range(4):
        idv = jnp.where(row8 == t, ids[t // 2, t % 2], idv)
    digits = jnp.where(lane8 == 0, idv >> 16, jnp.where(lane8 == 1, (idv >> 8) & 255, idv & 255))
    meta[...] = jnp.where(lane8 < 3, digits, 0).astype(F32)
    pl.semaphore_wait(barrier, len(partners))

    started = []

    def send(src, dst, ssem, rsem, dev, keep=True):
        copy = pltpu.make_async_remote_copy(
            src_ref=src, dst_ref=dst, send_sem=ssem, recv_sem=rsem, device_id=dev, device_id_type=MESH
        )
        copy.start()
        if keep:
            started.append(copy)

    def take(ref, sem):
        pltpu.make_async_copy(ref, ref, sem).wait()

    def take_tiles(n, sem):
        take(bbuf.at[pl.ds(0, n)], sem)

    for d in range(1, nx):
        send(hid, gath.at[x], g_send.at[d - 1], g_recv, {AXX: at(x, d, nx)})
    for d in range(1, nx):
        send(meta, gmeta.at[x], m_send, m_recv, {AXX: at(x, d, nx)}, keep=False)
    send(whbm, wmat.at[:, pl.ds(voc, voc)], w_send, w_recv, {AXC: 1 - c})

    gath[x] = hid[...]
    gmeta[x] = meta[...]

    for load in loads[2:5]:
        load.wait()
    rewards = []
    for r in range(2):
        both = sum(
            hid[r, :, pl.ds(k * LANES, LANES)].astype(F32) * rhead[k:k + 1].astype(F32)
            for k in range(rhead.shape[0])
        )
        both = jnp.sum(both, axis=1, keepdims=True)
        rewards.append(jnp.where(lens[r] == 1, both[0:1], both[1:2]))
    lane1 = lax.broadcasted_iota(jnp.int32, (1, LANES), 1)
    stacked = jnp.zeros((1, LANES), F32)
    for r in range(2):
        stacked += jnp.where(lane1 == pids[r], rewards[r], 0.0)
        stacked += jnp.where(lane1 == pids[r] + PROMPTS, rewards[r] * rewards[r], 0.0)
    pair[...] = jnp.where(row8 == 3, stacked, 0.0)

    take(gath.at[pl.ds(0, nx - 1)], g_recv)
    take(gmeta.at[pl.ds(0, nx - 1)], m_recv)

    whole = jnp.concatenate(
        [gath[i, r].astype(F32) for i in range(nx) for r in range(2)], axis=0
    ).astype(jnp.bfloat16)
    pieces = [whole[:, k * LANES:(k + 1) * LANES] for k in range(ka + kb + nx * kq)]
    for k in range(nx * kq):
        quarter[k // kq, k % kq] = pieces[ka + kb + k]
    base_a, base_b, base_o = (y * nz + z) * (ka + 1), (y * nz + z) * kb, (y * nz + z) * kq
    for k in range(ka):
        abuf[base_a + k] = pieces[k]
    for k in range(kb):
        bbuf[base_b + k] = pieces[ka + k]
    abuf[base_a + ka] = jnp.concatenate([gmeta[i, 0:4] for i in range(nx)], axis=0).astype(jnp.bfloat16)
    for k in range(kq):
        own[base_o + k] = quarter[x, k]

    send(pair, pgot, p_send, p_recv, {AXC: 1 - c})

    groups = [(dy % ny, dz % nz) for dy in ring_offsets(ny) for dz in ring_offsets(nz)]
    many = len(groups)
    where = {g: (at(y, g[0], ny), at(z, g[1], nz)) for g in groups}
    flat = {g: qy * nz + qz for g, (qy, qz) in where.items()}
    tiles_of = {"a": ka + 1, "b": kb, "c": kq}
    store = {"a": abuf, "b": bbuf, "c": own}
    out_sem = {"a": a_send, "b": b_send, "c": o_send}
    axis = {"x": (AXX, x, nx), "y": (AXY, y, ny), "z": (AXZ, z, nz)}
    index = {event: i for i, event in enumerate(sorted(need, key=str))}
    part_of = {g: n for n, op in enumerate([op for op in steps if op[0] == "last"]) for g in op[1]}

    def in_a(g, k=0):
        return flat[g] * (ka + 1) + k

    def in_b(g, k=0):
        return flat[g] * kb + k

    def in_c(r, g, k=0):
        return (r * many + flat[g]) * kq + k

    def block(colour, g):
        n = tiles_of[colour]
        return store[colour].at[pl.ds(flat[g] * n, n)]

    def put(link, event, g):
        name, pos, n = axis[link[0]]
        dev = {name: at(pos, 1 if link[1] == "+" else -1, n)}
        side_in = "+-".index(link[1])
        if event[0] == "x1":
            there = cbuf.at[pl.ds(in_c(side_in, g), kq)]
            send(block("c", g), there, c_send, e_recv.at[index[event]], dev, keep=False)
        elif event[0] == "x2":
            here, there = cbuf.at[pl.ds(in_c(side_in, g), kq)], cbuf.at[pl.ds(in_c(2, g), kq)]
            send(here, there, c_send, d_recv.at[part_of[g]], dev, keep=False)
        else:
            b = block(event[1], g)
            send(b, b, out_sem[event[1]], e_recv.at[index[event]], dev, keep=False)

    def get(event):
        take_tiles(need[event] * tiles_of["c" if event[0] == "x1" else event[1]], e_recv.at[index[event]])

    wide = 2 * LANES
    chip = ((y * nz + z) * nx + x) * 2
    turns = [at(x, off, nx) for off in (0, -1, 1, 2)]
    starts = [pl.multiple_of((ka + kb + q * kq) * LANES, LANES) for q in turns]

    def product(chunk, last):
        def step(n, carry):
            cols = pl.ds(n * wide, wide)
            left = []
            for i in chunk:
                if last:
                    parts = [own[flat[i] * kq + k] for k in range(kq)]
                    parts += [cbuf[in_c(r, i, k)] for r in range(3) for k in range(kq)]
                else:
                    parts = [abuf[in_a(i, k)] for k in range(ka)]
                    parts += [bbuf[in_b(i, k)] for k in range(kb)]
                left.append(jnp.concatenate(parts, axis=1))
            left = jnp.concatenate(left, axis=0)
            if last:
                right = jnp.concatenate([wmat[pl.ds(s, kq * LANES), cols] for s in starts], axis=0)
            else:
                right = wmat[pl.ds(0, (ka + kb) * LANES), cols]
            part = jnp.dot(left, right, preferred_element_type=F32)
            for m, i in enumerate(chunk):
                piece = part[m * rows:(m + 1) * rows]
                if last:
                    piece = acc[where[i] + (slice(None), cols)] + piece
                acc[where[i] + (slice(None), cols)] = piece
            return carry

        for n in range(2 * voc // wide):
            step(n, 0)

    def score(chunk):
        toks = len(chunk) * rows

        def logits():
            return jnp.concatenate([acc[where[i]] for i in chunk], axis=0)

        lane = lax.broadcasted_iota(jnp.int32, (toks, 2 * voc), 1)
        entry = jnp.where(lane < voc, (chip + c) * voc + lane, (chip + 1 - c) * voc + lane - voc)
        lane_t = lax.broadcasted_iota(jnp.int32, (toks, LANES), 1)
        peak = jnp.max(logits(), axis=1, keepdims=True)
        total = jnp.sum(jnp.exp(logits() - peak), axis=1, keepdims=True)
        dig = jnp.concatenate([abuf[in_a(i, ka)] for i in chunk], axis=0).astype(F32)
        want = (dig[:, 0:1] * 65536.0 + dig[:, 1:2] * 256.0 + dig[:, 2:3]).astype(jnp.int32)
        picked = jnp.sum(jnp.where(entry == want, logits(), 0.0), axis=1, keepdims=True)
        out = jnp.where(lane_t == 0, peak, jnp.where(lane_t == 1, total, jnp.where(lane_t == 2, picked, 0.0)))
        for m, i in enumerate(chunk):
            side[where[i][1], where[i][0]] = out[m * rows:(m + 1) * rows]

    ready = False
    count = 0
    for op in steps:
        if op[0] == "send":
            put(*op[1:])
        elif op[0] == "take":
            get(op[1])
        elif op[0] == "first":
            if not ready:
                loads[5].wait()
                take(wmat.at[:, pl.ds(voc, voc)], w_recv)
                ready = True
            product(op[1], False)
            count += 1
        else:
            take_tiles(len(op[1]) * kq, d_recv.at[part_of[op[1][0]]])
            product(op[1], True)
            score(op[1])
            count += 1

    take(pgot, p_recv)
    prompt_row = pair[...] + pgot[...]

    def slab(q):
        block = side[q].reshape(ny * rows, LANES)
        if ny * rows < LANES:
            block = jnp.concatenate([block, jnp.zeros((LANES - ny * rows, LANES), F32)], axis=0)
        return jnp.where(row8 == 3, prompt_row, block.T[0:8, :])

    def step(i, carry):
        h = (i + 1) // 2
        d = nz // 2 + h * (1 - 2 * (i % 2))
        q = lax.rem(z + d, nz)
        tiles[i] = slab(q)
        pltpu.make_async_remote_copy(
            src_ref=tiles.at[i], dst_ref=got_z.at[i], send_sem=z_send, recv_sem=z_recv,
            device_id={AXZ: q}, device_id_type=MESH,
        ).start()
        return carry

    lax.fori_loop(0, nz - 1, step, 0)

    def merge(parts):
        row8 = lax.broadcasted_iota(jnp.int32, parts[0].shape, 0)
        top = functools.reduce(jnp.maximum, [p[0:1] for p in parts])
        out = sum(p * jnp.where(row8 == 1, jnp.exp(p[0:1] - top), 1.0) for p in parts)
        return jnp.where(row8 == 0, top, out)

    mine = slab(z)
    take(got_z, z_recv)
    sums[...] = merge([mine] + [got_z[i] for i in range(nz - 1)])[0:4]
    others = [(dy, dx) for dy in range(ny) for dx in range(nx) if dy or dx]
    for n, (dy, dx) in sorted(enumerate(others), key=lambda o: -hops(ny, o[1][0]) - hops(nx, o[1][1])):
        send(sums, got_yx.at[n], y_send, y_recv, {AXY: at(y, dy, ny), AXX: at(x, dx, nx)}, keep=False)
    take(got_yx, y_recv)
    done = merge([sums[...]] + [got_yx[n] for n in range(len(others))])

    logprob = done[2:3] - (done[0:1] + jnp.log(done[1:2]))
    base = y * rows + x * 4
    r_out = lax.broadcasted_iota(jnp.int32, (2, 2), 0)
    w_out = lax.broadcasted_iota(jnp.int32, (2, 2), 1)
    value = jnp.zeros((2, 2), F32)
    for t in range(4):
        r, w = t // 2, t % 2
        one = jnp.sum(jnp.where(lane1 == base + t, logprob, 0.0), axis=1, keepdims=True)
        one = jnp.where(w < lens[r], one, 0.0)
        value = jnp.where((r_out == r) & (w_out == w), one, value)
    out1[...] = value
    moment = done[3:4] * (1.0 / GROUP)
    spot = lax.broadcasted_iota(jnp.int32, (1, 2), 1)
    adv = jnp.zeros((1, 2), F32)
    for r in range(2):
        mean = jnp.sum(jnp.where(lane1 == pids[r], moment, 0.0), axis=1, keepdims=True)
        square = jnp.sum(jnp.where(lane1 == pids[r] + PROMPTS, moment, 0.0), axis=1, keepdims=True)
        scale = jnp.sqrt(jnp.maximum(square - mean * mean, 1.0))
        adv = jnp.where(spot == r, (rewards[r] - mean) / scale, adv)
    out2[...] = adv

    for copy in started:
        copy.wait_send()
    take_tiles((many - 1) * (ka + 1), a_send)
    take_tiles((many - 1) * kq, o_send)
    take_tiles((many - 1) * kb, b_send)
    take(cbuf, c_send)
    take_tiles(nz - 1, z_send)
    take_tiles(nx - 1, m_send)
    take(got_yx, y_send)


def local(hidden, lm_head, reward_head, target_ids, lengths, prompt_ids):
    nx, ny, nz = (lax.axis_size(a) for a in (AXX, AXY, AXZ))
    width, voc = lm_head.shape
    tiles = width // LANES
    kq = max(1, tiles * 3 // (7 * nx))
    ka = max(1, (tiles - kq * nx) * 5 // 16)
    kb = tiles - kq * nx - ka
    rows = nx * 4
    size = rows * LANES * 2
    steps, need = plan(ny, nz, {"a": (ka + 1) * size, "b": kb * size, "c": kq * size})
    lasts = sum(op[0] == "last" for op in steps)
    dma = pltpu.SemaphoreType.DMA
    vmem = pl.BlockSpec(memory_space=pltpu.VMEM)
    tile = (8, LANES)
    out1, out2 = pl.pallas_call(
        functools.partial(kernel, (nx, ny, nz, ka, kb, kq), steps, need),
        out_shape=(pltpu.VMEM((2, 2), F32), pltpu.VMEM((1, 2), F32)),
        in_specs=[pl.BlockSpec(memory_space=pl.ANY)] * 6,
        out_specs=(vmem, vmem),
        scratch_shapes=[
            pltpu.VMEM((2, 2, width), jnp.bfloat16),
            pltpu.VMEM((tiles, LANES), jnp.bfloat16),
            pltpu.SMEM((2, 2), jnp.int32),
            pltpu.SMEM((2,), jnp.int32),
            pltpu.SMEM((2,), jnp.int32),
            pltpu.VMEM((width, 2 * voc), jnp.bfloat16),
            pltpu.VMEM((ny * nz * (ka + 1), rows, LANES), jnp.bfloat16),
            pltpu.VMEM((ny * nz * kb, rows, LANES), jnp.bfloat16),
            pltpu.VMEM((ny * nz * kq, rows, LANES), jnp.bfloat16),
            pltpu.VMEM((3 * ny * nz * kq, rows, LANES), jnp.bfloat16),
            pltpu.VMEM((nx, kq, rows, LANES), jnp.bfloat16),
            pltpu.VMEM((ny, nz, rows, 2 * voc), F32),
            pltpu.VMEM((nz, ny, rows, LANES), F32),
            pltpu.VMEM((nx, 2, 2, width), jnp.bfloat16),
            pltpu.VMEM((nx,) + tile, F32),
            pltpu.VMEM(tile, F32),
            pltpu.VMEM((nz - 1,) + tile, F32),
            pltpu.VMEM((nz - 1,) + tile, F32),
            pltpu.VMEM((ny * nx - 1, 4, LANES), F32),
            pltpu.VMEM((4, LANES), F32),
            pltpu.VMEM(tile, F32),
            pltpu.VMEM(tile, F32),
            dma((6,)), dma, dma,
            dma((nx - 1,)), dma, dma, dma,
            dma, dma,
            dma, dma, dma, dma, dma((len(need),)), dma((lasts,)),
            dma, dma, dma, dma,
        ],
        compiler_params=pltpu.CompilerParams(collective_id=0, has_side_effects=True),
        name="gather_score",
    )(hidden, lm_head, reward_head.reshape(tiles, LANES), target_ids, lengths, prompt_ids)
    return out1, out2.reshape(2)


def solution(mesh):
    split = Mesh(mesh.devices.reshape(mesh.shape["rep"], 8, 4, 2), REP_DP)
    placed = (P(REP_DP, None, None), P(None, REP_DP), P(), P(REP_DP, None), P(REP_DP), P(REP_DP))
    return jax.shard_map(
        local, mesh=split, in_specs=placed, out_specs=(P(REP_DP, None), P(REP_DP)), check_vma=False
    )
```

```python
import functools

import jax
import jax.numpy as jnp
from jax import lax
from jax.experimental import pallas as pl
from jax.experimental.pallas import tpu as pltpu
from jax.sharding import Mesh
from jax.sharding import PartitionSpec as P

GROUP = 16
PROMPTS = 64
REP_DP = ("rep", "dp_0", "dp_1", "dp_2")
AXY, AXZ, AXX, AXC = REP_DP
LANES = 128
MESH = pl.DeviceIdType.MESH
F32 = jnp.float32


def ring_offsets(n):
    order = [0]
    for d in range(1, n // 2 + 1):
        order.append(-d)
        if 2 * d < n:
            order.append(d)
    return order


def hops(n, off):
    return min(off % n, -off % n)


def plan(ny, nz, sizes, depth=1.2, rate=46.6e3, lag=2.2, least=(12, 8), most=16, tail=24):
    parts = {"a": (0, ny, nz), "b": (1, nz, ny), "c": (0, ny, nz)}
    groups = [(dy % ny, dz % nz) for dy in ring_offsets(ny) for dz in ring_offsets(nz)]
    now, free, pending, issued, arrive = [0.0], {}, {}, {}, {}
    ops = []
    extra = {"a": 0, "b": 0, "c": 2}

    def queue(link, left, colour, event, what):
        pending.setdefault(link, []).append((-left, len(ops), colour, event, what))

    def issue():
        for link, wait in sorted(pending.items()):
            while wait and free.get(link, 0.0) - now[0] < depth:
                wait.sort(key=lambda w: w[0])
                left, _, colour, event, what = wait.pop(0)
                start = max(now[0], free.get(link, 0.0))
                free[link] = start + sizes[colour] / rate
                arrive[event] = max(arrive.get(event, 0.0), free[link] + lag)
                issued[event] = issued.get(event, 0) + 1
                ops.append(("send", link, event, what, colour))
                now[0] += 0.015

    def place(colour, off1, off2):
        swap, n1, n2 = parts[colour]
        return (off2 % n2, off1 % n1) if swap else (off1 % n1, off2 % n2)

    def ways(n, d):
        return (1, -1) if 2 * d < n else (1,)

    need, outstanding = {}, set()

    def put1(colour, d, way):
        swap, n1, n2 = parts[colour]
        if d <= n1 // 2 and way in ways(n1, d):
            event = ("p1", both[colour], d)
            need[event] = len(ways(n1, d)) * len(both[colour])
            outstanding.add(event)
            queue(("zy" if swap else "yz")[0] + "+-"[way < 0], n1 // 2 - d + n2 // 2 + extra[colour], colour, event,
                  place(colour, -way * (d - 1), 0))

    def put2(colour, j, d, way):
        swap, n1, n2 = parts[colour]
        if d > n2 // 2:
            return
        if 2 * d == n2 and way != (1 if j % 4 in (0, 3) else -1):
            return
        event = ("p2", both[colour], j, d)
        need[event] = (2 if 2 * d < n2 else 1) * len(both[colour])
        outstanding.add(event)
        queue(("zy" if swap else "yz")[1] + "+-"[way < 0], n2 // 2 - d + extra[colour], colour, event,
              place(colour, ring_offsets(n1)[j], -way * (d - 1)))

    have = {c: set() for c in "abc"}
    batch, done = {}, []
    both = {"a": "ab", "b": "ab", "c": "c"}

    def got(colour, new):
        have[colour].update(new)
        if colour == "c":
            event = ("x1",) + new[0]
            need[event] = 2 * len(new)
            batch[event] = new
            outstanding.add(event)
            for g in new:
                for way in "+-":
                    queue("x" + way, 1, "c", event, g)

    def take(event):
        if event[0] == "x1":
            for n, g in enumerate(batch[event]):
                queue("x" + "+-"[(n + len(done)) % 2], 0, "c", ("x2", g), g)
            done.append(event)
            return
        for colour in event[1]:
            pass_on(event, colour)

    def pass_on(event, colour):
        swap, n1, n2 = parts[colour]
        if event[0] == "p1":
            d = event[2]
            for way in ways(n1, d):
                put1(colour, d + 1, way)
                j = [o % n1 for o in ring_offsets(n1)].index(-way * d % n1)
                for w2 in (1, -1):
                    put2(colour, j, 1, w2)
            got(colour, [place(colour, -way * d, 0) for way in ways(n1, d)])
        else:
            j, d = event[2:]
            sides = (1, -1) if 2 * d < n2 else ((1 if j % 4 in (0, 3) else -1),)
            for way in sides:
                put2(colour, j, d + 1, way)
            got(colour, [place(colour, ring_offsets(n1)[j], -way * d) for way in sides])

    for colour in "cab":
        for way in (1, -1):
            put1(colour, 1, way)
        for way in (1, -1):
            put2(colour, 0, 1, way)
        got(colour, [(0, 0)])
    first_done, last_done = [], []
    while len(last_done) < len(groups):
        issue()
        ready = [e for e in outstanding if issued.get(e, 0) == need[e]]
        ready.sort(key=lambda e: (arrive[e], str(e)))
        if ready and arrive[ready[0]] <= now[0]:
            event = ready[0]
            outstanding.discard(event)
            ops.append(("take", event))
            now[0] += 0.03
            take(event)
            continue
        left = [g for g in groups if g not in first_done]
        one = [g for g in left if g in have["a"] and g in have["b"]][:most]
        todo = [g for g in groups if g not in last_done]
        two = [g for g in first_done if g not in last_done and issued.get(("x2", g)) and arrive[("x2", g)] <= now[0]][:most]
        if one and (len(one) >= least[len(left) <= tail] or len(one) == len(left)) and not (two and len(two) >= least[len(todo) <= tail]):
            first_done.extend(one)
            ops.append(("first", tuple(one)))
            now[0] += 0.57 + 0.02 * len(one)
        elif two and (len(two) >= least[len(todo) <= tail] or len(two) == len(todo)):
            last_done.extend(two)
            ops.append(("last", tuple(two)))
            now[0] += 0.6 + 0.028 * len(two)
        elif ready:
            now[0] = arrive[ready[0]]
        else:
            late = [arrive[("x2", g)] for g in todo if issued.get(("x2", g)) and arrive[("x2", g)] > now[0]]
            nxt = min(late) if late else None
            if nxt is None:
                nxt = min(free[l] for l in pending if pending[l]) - depth + 1e-6
            now[0] = max(nxt, now[0])
    return ops, need


def kernel(
    sizes, steps, need, hid_in, whbm, rhead_in, ids_in, lens_in, pids_in, out1, out2,
    hid, rhead, ids, lens, pids,
    wmat, abuf, bbuf, own, cbuf, quarter, acc, side, gath, gmeta, meta, tiles, got_z, got_yx, sums, pair, pgot,
    in_sem, w_send, w_recv, g_send, g_recv, m_send, m_recv, p_send, p_recv,
    a_send, b_send, c_send, o_send, e_recv, d_recv, z_send, z_recv, y_send, y_recv,
):
    nx, ny, nz, ka, kb, kq = sizes
    rows = nx * 4
    voc = whbm.shape[1]
    y, z, x, c = (lax.axis_index(a) for a in (AXY, AXZ, AXX, AXC))

    def at(pos, off, n):
        return lax.rem(pos + (off % n), n)

    barrier = pltpu.get_barrier_semaphore()
    partners = [{AXX: at(x, d, nx)} for d in range(1, nx)]
    partners += [{AXY: at(y, d, ny)} for d in (1, -1)]
    partners += [{AXZ: at(z, d, nz)} for d in (1, -1)]
    partners += [{AXC: 1 - c}]
    for dev in partners:
        pl.semaphore_signal(barrier, inc=1, device_id=dev, device_id_type=MESH)

    loads = [
        pltpu.make_async_copy(src, dst, in_sem.at[i])
        for i, (src, dst) in enumerate((
            (hid_in, hid), (ids_in, ids), (lens_in, lens), (pids_in, pids), (rhead_in, rhead),
            (whbm, wmat.at[:, pl.ds(0, voc)]),
        ))
    ]
    for load in loads:
        load.start()
    loads[0].wait()
    loads[1].wait()

    row8 = lax.broadcasted_iota(jnp.int32, (8, LANES), 0)
    lane8 = lax.broadcasted_iota(jnp.int32, (8, LANES), 1)
    idv = jnp.zeros((8, LANES), jnp.int32)
    for t in range(4):
        idv = jnp.where(row8 == t, ids[t // 2, t % 2], idv)
    digits = jnp.where(lane8 == 0, idv >> 16, jnp.where(lane8 == 1, (idv >> 8) & 255, idv & 255))
    meta[...] = jnp.where(lane8 < 3, digits, 0).astype(F32)
    pl.semaphore_wait(barrier, len(partners))

    started = []

    def send(src, dst, ssem, rsem, dev, keep=True):
        copy = pltpu.make_async_remote_copy(
            src_ref=src, dst_ref=dst, send_sem=ssem, recv_sem=rsem, device_id=dev, device_id_type=MESH
        )
        copy.start()
        if keep:
            started.append(copy)

    def take(ref, sem):
        pltpu.make_async_copy(ref, ref, sem).wait()

    def take_tiles(n, sem):
        take(bbuf.at[pl.ds(0, n)], sem)

    for d in range(1, nx):
        send(hid, gath.at[x], g_send.at[d - 1], g_recv, {AXX: at(x, d, nx)})
    for d in range(1, nx):
        send(meta, gmeta.at[x], m_send, m_recv, {AXX: at(x, d, nx)}, keep=False)
    send(whbm, wmat.at[:, pl.ds(voc, voc)], w_send, w_recv, {AXC: 1 - c})

    gath[x] = hid[...]
    gmeta[x] = meta[...]

    for load in loads[2:5]:
        load.wait()
    rewards = []
    for r in range(2):
        both = sum(
            hid[r, :, pl.ds(k * LANES, LANES)].astype(F32) * rhead[k:k + 1].astype(F32)
            for k in range(rhead.shape[0])
        )
        both = jnp.sum(both, axis=1, keepdims=True)
        rewards.append(jnp.where(lens[r] == 1, both[0:1], both[1:2]))
    lane1 = lax.broadcasted_iota(jnp.int32, (1, LANES), 1)
    stacked = jnp.zeros((1, LANES), F32)
    for r in range(2):
        stacked += jnp.where(lane1 == pids[r], rewards[r], 0.0)
        stacked += jnp.where(lane1 == pids[r] + PROMPTS, rewards[r] * rewards[r], 0.0)
    pair[...] = jnp.where(row8 == 3, stacked, 0.0)

    take(gath.at[pl.ds(0, nx - 1)], g_recv)
    take(gmeta.at[pl.ds(0, nx - 1)], m_recv)

    whole = jnp.concatenate(
        [gath[i, r].astype(F32) for i in range(nx) for r in range(2)], axis=0
    ).astype(jnp.bfloat16)
    pieces = [whole[:, k * LANES:(k + 1) * LANES] for k in range(ka + kb + nx * kq)]
    for k in range(nx * kq):
        quarter[k // kq, k % kq] = pieces[ka + kb + k]
    base_a, base_b, base_o = (y * nz + z) * (ka + 1), (y * nz + z) * kb, (y * nz + z) * kq
    for k in range(ka):
        abuf[base_a + k] = pieces[k]
    for k in range(kb):
        bbuf[base_b + k] = pieces[ka + k]
    abuf[base_a + ka] = jnp.concatenate([gmeta[i, 0:4] for i in range(nx)], axis=0).astype(jnp.bfloat16)
    for k in range(kq):
        own[base_o + k] = quarter[x, k]

    send(pair, pgot, p_send, p_recv, {AXC: 1 - c})

    groups = [(dy % ny, dz % nz) for dy in ring_offsets(ny) for dz in ring_offsets(nz)]
    many = len(groups)
    where = {g: (at(y, g[0], ny), at(z, g[1], nz)) for g in groups}
    flat = {g: qy * nz + qz for g, (qy, qz) in where.items()}
    tiles_of = {"a": ka + 1, "b": kb, "c": kq}
    store = {"a": abuf, "b": bbuf, "c": own}
    out_sem = {"a": a_send, "b": b_send, "c": o_send}
    axis = {"x": (AXX, x, nx), "y": (AXY, y, ny), "z": (AXZ, z, nz)}
    index = {event: i for i, event in enumerate(sorted(need, key=str))}
    part_of = {g: n for n, op in enumerate([op for op in steps if op[0] == "last"]) for g in op[1]}

    def in_a(g, k=0):
        return flat[g] * (ka + 1) + k

    def in_b(g, k=0):
        return flat[g] * kb + k

    def in_c(r, g, k=0):
        return (r * many + flat[g]) * kq + k

    def block(colour, g):
        n = tiles_of[colour]
        return store[colour].at[pl.ds(flat[g] * n, n)]

    def put(link, event, g, colour):
        name, pos, n = axis[link[0]]
        dev = {name: at(pos, 1 if link[1] == "+" else -1, n)}
        side_in = "+-".index(link[1])
        if event[0] == "x1":
            there = cbuf.at[pl.ds(in_c(side_in, g), kq)]
            send(block("c", g), there, c_send, e_recv.at[index[event]], dev, keep=False)
        elif event[0] == "x2":
            here, there = cbuf.at[pl.ds(in_c(side_in, g), kq)], cbuf.at[pl.ds(in_c(2, g), kq)]
            send(here, there, c_send, d_recv.at[part_of[g]], dev, keep=False)
        else:
            b = block(colour, g)
            send(b, b, out_sem[colour], e_recv.at[index[event]], dev, keep=False)

    def get(event):
        kinds = "c" if event[0] == "x1" else event[1]
        take_tiles(need[event] * sum(tiles_of[k] for k in kinds) // len(kinds), e_recv.at[index[event]])

    wide = 2 * LANES
    chip = ((y * nz + z) * nx + x) * 2
    turns = [at(x, off, nx) for off in (0, -1, 1, 2)]
    starts = [pl.multiple_of((ka + kb + q * kq) * LANES, LANES) for q in turns]

    def product(chunk, last):
        def step(n, carry):
            cols = pl.ds(n * wide, wide)
            left = []
            for i in chunk:
                if last:
                    parts = [own[flat[i] * kq + k] for k in range(kq)]
                    parts += [cbuf[in_c(r, i, k)] for r in range(3) for k in range(kq)]
                else:
                    parts = [abuf[in_a(i, k)] for k in range(ka)]
                    parts += [bbuf[in_b(i, k)] for k in range(kb)]
                left.append(jnp.concatenate(parts, axis=1))
            left = jnp.concatenate(left, axis=0)
            if last:
                right = jnp.concatenate([wmat[pl.ds(s, kq * LANES), cols] for s in starts], axis=0)
            else:
                right = wmat[pl.ds(0, (ka + kb) * LANES), cols]
            part = jnp.dot(left, right, preferred_element_type=F32)
            for m, i in enumerate(chunk):
                piece = part[m * rows:(m + 1) * rows]
                if last:
                    piece = acc[where[i] + (slice(None), cols)] + piece
                acc[where[i] + (slice(None), cols)] = piece
            return carry

        for n in range(2 * voc // wide):
            step(n, 0)

    def score(chunk):
        toks = len(chunk) * rows

        def logits():
            return jnp.concatenate([acc[where[i]] for i in chunk], axis=0)

        lane = lax.broadcasted_iota(jnp.int32, (toks, 2 * voc), 1)
        entry = jnp.where(lane < voc, (chip + c) * voc + lane, (chip + 1 - c) * voc + lane - voc)
        lane_t = lax.broadcasted_iota(jnp.int32, (toks, LANES), 1)
        peak = jnp.max(logits(), axis=1, keepdims=True)
        total = jnp.sum(jnp.exp(logits() - peak), axis=1, keepdims=True)
        dig = jnp.concatenate([abuf[in_a(i, ka)] for i in chunk], axis=0).astype(F32)
        want = (dig[:, 0:1] * 65536.0 + dig[:, 1:2] * 256.0 + dig[:, 2:3]).astype(jnp.int32)
        picked = jnp.sum(jnp.where(entry == want, logits(), 0.0), axis=1, keepdims=True)
        out = jnp.where(lane_t == 0, peak, jnp.where(lane_t == 1, total, jnp.where(lane_t == 2, picked, 0.0)))
        for m, i in enumerate(chunk):
            side[where[i][1], where[i][0]] = out[m * rows:(m + 1) * rows]

    ready = False
    count = 0
    for op in steps:
        if op[0] == "send":
            put(*op[1:])
        elif op[0] == "take":
            get(op[1])
        elif op[0] == "first":
            if not ready:
                loads[5].wait()
                take(wmat.at[:, pl.ds(voc, voc)], w_recv)
                ready = True
            product(op[1], False)
            count += 1
        else:
            take_tiles(len(op[1]) * kq, d_recv.at[part_of[op[1][0]]])
            product(op[1], True)
            score(op[1])
            count += 1

    take(pgot, p_recv)
    prompt_row = pair[...] + pgot[...]

    def slab(q):
        block = side[q].reshape(ny * rows, LANES)
        if ny * rows < LANES:
            block = jnp.concatenate([block, jnp.zeros((LANES - ny * rows, LANES), F32)], axis=0)
        return jnp.where(row8 == 3, prompt_row, block.T[0:8, :])

    def step(i, carry):
        h = (i + 1) // 2
        d = nz // 2 + h * (1 - 2 * (i % 2))
        q = lax.rem(z + d, nz)
        tiles[i] = slab(q)
        pltpu.make_async_remote_copy(
            src_ref=tiles.at[i], dst_ref=got_z.at[i], send_sem=z_send, recv_sem=z_recv,
            device_id={AXZ: q}, device_id_type=MESH,
        ).start()
        return carry

    lax.fori_loop(0, nz - 1, step, 0)

    def merge(parts):
        row8 = lax.broadcasted_iota(jnp.int32, parts[0].shape, 0)
        top = functools.reduce(jnp.maximum, [p[0:1] for p in parts])
        out = sum(p * jnp.where(row8 == 1, jnp.exp(p[0:1] - top), 1.0) for p in parts)
        return jnp.where(row8 == 0, top, out)

    mine = slab(z)
    take(got_z, z_recv)
    sums[...] = merge([mine] + [got_z[i] for i in range(nz - 1)])[0:4]
    others = [(dy, dx) for dy in range(ny) for dx in range(nx) if dy or dx]
    for n, (dy, dx) in sorted(enumerate(others), key=lambda o: -hops(ny, o[1][0]) - hops(nx, o[1][1])):
        send(sums, got_yx.at[n], y_send, y_recv, {AXY: at(y, dy, ny), AXX: at(x, dx, nx)}, keep=False)
    take(got_yx, y_recv)
    done = merge([sums[...]] + [got_yx[n] for n in range(len(others))])

    logprob = done[2:3] - (done[0:1] + jnp.log(done[1:2]))
    base = y * rows + x * 4
    r_out = lax.broadcasted_iota(jnp.int32, (2, 2), 0)
    w_out = lax.broadcasted_iota(jnp.int32, (2, 2), 1)
    value = jnp.zeros((2, 2), F32)
    for t in range(4):
        r, w = t // 2, t % 2
        one = jnp.sum(jnp.where(lane1 == base + t, logprob, 0.0), axis=1, keepdims=True)
        one = jnp.where(w < lens[r], one, 0.0)
        value = jnp.where((r_out == r) & (w_out == w), one, value)
    out1[...] = value
    moment = done[3:4] * (1.0 / GROUP)
    spot = lax.broadcasted_iota(jnp.int32, (1, 2), 1)
    adv = jnp.zeros((1, 2), F32)
    for r in range(2):
        mean = jnp.sum(jnp.where(lane1 == pids[r], moment, 0.0), axis=1, keepdims=True)
        square = jnp.sum(jnp.where(lane1 == pids[r] + PROMPTS, moment, 0.0), axis=1, keepdims=True)
        scale = jnp.sqrt(jnp.maximum(square - mean * mean, 1.0))
        adv = jnp.where(spot == r, (rewards[r] - mean) / scale, adv)
    out2[...] = adv

    for copy in started:
        copy.wait_send()
    take_tiles((many - 1) * (ka + 1), a_send)
    take_tiles((many - 1) * kq, o_send)
    take_tiles((many - 1) * kb, b_send)
    take(cbuf, c_send)
    take_tiles(nz - 1, z_send)
    take_tiles(nx - 1, m_send)
    take(got_yx, y_send)


def local(hidden, lm_head, reward_head, target_ids, lengths, prompt_ids):
    nx, ny, nz = (lax.axis_size(a) for a in (AXX, AXY, AXZ))
    width, voc = lm_head.shape
    tiles = width // LANES
    kq = max(1, tiles * 3 // (7 * nx))
    ka = max(1, (tiles - kq * nx) * 5 // 16)
    kb = tiles - kq * nx - ka
    rows = nx * 4
    size = rows * LANES * 2
    steps, need = plan(ny, nz, {"a": (ka + 1) * size, "b": kb * size, "c": kq * size})
    lasts = sum(op[0] == "last" for op in steps)
    dma = pltpu.SemaphoreType.DMA
    vmem = pl.BlockSpec(memory_space=pltpu.VMEM)
    tile = (8, LANES)
    out1, out2 = pl.pallas_call(
        functools.partial(kernel, (nx, ny, nz, ka, kb, kq), steps, need),
        out_shape=(pltpu.VMEM((2, 2), F32), pltpu.VMEM((1, 2), F32)),
        in_specs=[pl.BlockSpec(memory_space=pl.ANY)] * 6,
        out_specs=(vmem, vmem),
        scratch_shapes=[
            pltpu.VMEM((2, 2, width), jnp.bfloat16),
            pltpu.VMEM((tiles, LANES), jnp.bfloat16),
            pltpu.SMEM((2, 2), jnp.int32),
            pltpu.SMEM((2,), jnp.int32),
            pltpu.SMEM((2,), jnp.int32),
            pltpu.VMEM((width, 2 * voc), jnp.bfloat16),
            pltpu.VMEM((ny * nz * (ka + 1), rows, LANES), jnp.bfloat16),
            pltpu.VMEM((ny * nz * kb, rows, LANES), jnp.bfloat16),
            pltpu.VMEM((ny * nz * kq, rows, LANES), jnp.bfloat16),
            pltpu.VMEM((3 * ny * nz * kq, rows, LANES), jnp.bfloat16),
            pltpu.VMEM((nx, kq, rows, LANES), jnp.bfloat16),
            pltpu.VMEM((ny, nz, rows, 2 * voc), F32),
            pltpu.VMEM((nz, ny, rows, LANES), F32),
            pltpu.VMEM((nx, 2, 2, width), jnp.bfloat16),
            pltpu.VMEM((nx,) + tile, F32),
            pltpu.VMEM(tile, F32),
            pltpu.VMEM((nz - 1,) + tile, F32),
            pltpu.VMEM((nz - 1,) + tile, F32),
            pltpu.VMEM((ny * nx - 1, 4, LANES), F32),
            pltpu.VMEM((4, LANES), F32),
            pltpu.VMEM(tile, F32),
            pltpu.VMEM(tile, F32),
            dma((6,)), dma, dma,
            dma((nx - 1,)), dma, dma, dma,
            dma, dma,
            dma, dma, dma, dma, dma((len(need),)), dma((lasts,)),
            dma, dma, dma, dma,
        ],
        compiler_params=pltpu.CompilerParams(collective_id=0, has_side_effects=True),
        name="gather_score",
    )(hidden, lm_head, reward_head.reshape(tiles, LANES), target_ids, lengths, prompt_ids)
    return out1, out2.reshape(2)


def solution(mesh):
    split = Mesh(mesh.devices.reshape(mesh.shape["rep"], 8, 4, 2), REP_DP)
    placed = (P(REP_DP, None, None), P(None, REP_DP), P(), P(REP_DP, None), P(REP_DP), P(REP_DP))
    return jax.shard_map(
        local, mesh=split, in_specs=placed, out_specs=(P(REP_DP, None), P(REP_DP)), check_vma=False
    )
```
